32 devices in a mesh: section: 4 (over y, x), seq: 8 (over z, core).
Axes of the slice: x: 2, y: 2, z: 4, core: 2. Of those that a mesh axis runs over, the one named last changes fastest.
Arguments:
- queries: bfloat16 [4, 1024, 4096], P('section', 'seq'), may hold values from -500 to 500
- keys: bfloat16 [4, 1024, 512], P('section', 'seq'), may hold values from -6 to 6
- values: bfloat16 [4, 1024, 512], P('section', 'seq'), may hold values from -6 to 6
- out_grad: bfloat16 [4, 1024, 4096], P('section', 'seq'), may hold values from -6 to 6
- documents: int32 [4, 1024], P('section'), may hold values from 0 to 3, never falling along the last dimension, each value on 1 to 512 neighbouring positions
- query_weight: bfloat16 [4, 4096, 4096], P('section', 'seq'), may hold values from -0.09375 to 0.09375
- key_weight: bfloat16 [4, 512, 4096], P('section'), may hold values from -0.1875 to 0.1875
- value_weight: bfloat16 [4, 512, 4096], P('section'), may hold values from -0.1875 to 0.1875
Outputs:
- upstream: bfloat16 [4, 1024, 4096], P('section', 'seq')
The draws below stay inside these ranges and needn't reach their ends.
Inputs may be any that keep to these rules, and one draw needn't show every extreme that they name: `documents`: each section's document ids never fall along its tokens.
All inputs are finite; a program needn't handle non-finite values.
Results may differ from the reference program's by a relative error of at most 0.0058.
Values may be sent and summed in bfloat16 or wider, within the bound.
A program may use at most 192 MiB of HBM per device.

```python
import math
import jax
import jax.numpy as jnp
import numpy as np
from jax import lax

D = 4096
H = 32
KV = 4
HD = 128
SECTIONS = 4
TOKENS = 1024
N_SEQ = 8


def query_key_pair(key):
    base = jax.random.fold_in(key, 11)
    key_q, key_k = jax.random.split(base, 2)
    queries = jax.random.normal(key_q, (SECTIONS, TOKENS, H * HD), jnp.float32)
    keys = jax.random.normal(key_k, (SECTIONS, TOKENS, KV * HD), jnp.float32)
    keys = jnp.clip(keys, -6.0, 6.0)
    return (queries, keys)


def draw_queries(key, part):
    return query_key_pair(key)[0].astype(jnp.bfloat16)


def draw_keys(key, part):
    return query_key_pair(key)[1].astype(jnp.bfloat16)


def shard_levels(rng, shape, shards, least, top_value):
    def one(axis_at, parts):
        draws = jax.random.uniform(jax.random.fold_in(jax.random.fold_in(rng, 6), axis_at), (parts,), jnp.float32, least / len(shards), top_value / len(shards))
        return jnp.repeat(jnp.exp(draws), shape[axis_at] // parts).reshape((-1,) + (1,) * (len(shape) - axis_at - 1))

    loudness = one(*shards[0])
    for cut in shards[1:]:
        loudness = loudness * one(*cut)
    return loudness


def split_up(amount, total, most, slope):
    weights = [(1 << 20) // math.isqrt(rank ** slope) + 1 for rank in range(2, amount + 1)]
    rest, counts = total - most - (amount - 1), [1] * (amount - 1)
    while rest > 0:
        movable = [i for i in range(amount - 1) if counts[i] < most]
        pool, remaining = sum([weights[i] for i in movable]), rest
        for i in movable:
            extra = min(most - counts[i], max(1, remaining * weights[i] // pool), rest)
            counts[i] = counts[i] + extra
            rest = rest - extra
    return np.array([most] + counts)


def ragged(own_key, amount, total, bound, slope):
    if amount == 2:
        one = jax.random.randint(own_key, (), max(1, total - bound), min(bound, total - 1) + 1)
        return jnp.stack([one, total - one])
    tallies = jnp.asarray(split_up(amount, total, bound, slope), jnp.int32)
    twos = (amount - 1) // 2
    donor, taker = tallies[1:1 + 2 * twos:2], tallies[2:2 + 2 * twos:2]
    slack = jnp.minimum(donor - 1, bound - taker)
    passed = jax.random.randint(jax.random.fold_in(own_key, 1), (twos,), 0, 1 << 20) % (slack + 1)
    tallies = tallies.at[1:1 + 2 * twos:2].set(donor - passed).at[2:2 + 2 * twos:2].set(taker + passed)
    return tallies[jax.random.permutation(jax.random.fold_in(own_key, 2), amount)]


def normal_values(key, dims, deviation, reach, cuts=(), kind=jnp.bfloat16):
    loudness = shard_levels(key, dims, cuts, -0.22, 0.18) if cuts else 1.0
    array = jax.random.normal(key, dims, jnp.float32) * deviation * loudness
    return jnp.minimum(jnp.maximum(array, -reach), reach).astype(kind)


def setup_inputs(seed: int = 0) -> dict:
    streams_of = jax.random.split(jax.random.key(seed), 9)
    return {
        "queries": draw_queries(jax.random.fold_in(streams_of[8], 71), 0),
        "keys": draw_keys(jax.random.fold_in(streams_of[8], 71), 0),
        "values": normal_values(streams_of[2], (SECTIONS, TOKENS, KV * HD), 1.0, 6.0, ((0, 4), (1, 8))),
        "out_grad": normal_values(streams_of[3], (SECTIONS, TOKENS, H * HD), 1.0, 6.0, ((0, 4), (1, 8))),
        "documents": jax.vmap(lambda own: jnp.searchsorted(jnp.cumsum(ragged(own, 4, TOKENS, TOKENS // 2, 0)), jnp.arange(TOKENS), side="right"))(jax.random.split(streams_of[4], SECTIONS)).reshape((SECTIONS, TOKENS)).astype(jnp.int32),
        "query_weight": normal_values(streams_of[5], (SECTIONS, H * HD, D), (H * HD) ** -0.5, 0.09375, ((0, 4), (1, 8))),
        "key_weight": normal_values(streams_of[6], (SECTIONS, KV * HD, D), (N_SEQ * HD) ** -0.5, 0.1875, ((0, 4),)),
        "value_weight": normal_values(streams_of[7], (SECTIONS, KV * HD, D), (N_SEQ * HD) ** -0.5, 0.1875, ((0, 4),)),
    }


def slot_grads(index, q_all, k_all, v_all, o_all, ids):
    per = H // N_SEQ
    total = q_all.shape[0]
    kvh = index * KV // N_SEQ
    scale = 1.0 / math.sqrt(HD)
    q_blk = lax.dynamic_slice_in_dim(q_all, index * per * HD, per * HD, 1).reshape(total, per, HD).astype(jnp.float32)
    o_blk = lax.dynamic_slice_in_dim(o_all, index * per * HD, per * HD, 1).reshape(total, per, HD).astype(jnp.float32)
    k_head = lax.dynamic_slice_in_dim(k_all, kvh * HD, HD, 1).astype(jnp.float32)
    v_head = lax.dynamic_slice_in_dim(v_all, kvh * HD, HD, 1).astype(jnp.float32)
    rows = lax.iota(jnp.int32, total)
    allowed = (rows[None, :] <= rows[:, None]) & (ids[None, :] == ids[:, None])
    scores = jnp.einsum('bhd,td->hbt', q_blk, k_head) * scale
    scores = jnp.where(allowed[None], scores, -jnp.inf)
    top = lax.optimization_barrier(jnp.max(scores, axis=-1, keepdims=True))
    expo = jnp.exp(scores - top)
    prob = expo / lax.optimization_barrier(jnp.sum(expo, axis=-1, keepdims=True))
    prob_low = prob.astype(jnp.bfloat16)
    dprob = jnp.einsum('bhd,td->hbt', o_blk, v_head)
    delta = lax.optimization_barrier(jnp.sum(prob * dprob, axis=-1, keepdims=True))
    dscore = (prob * (dprob - delta) * scale).astype(jnp.bfloat16).astype(jnp.float32)
    dquery = jnp.einsum('hbt,td->bhd', dscore, k_head).astype(jnp.bfloat16).reshape(total, per * HD)
    dkey = jnp.einsum('hbt,bhd->td', dscore, q_blk).astype(jnp.bfloat16)
    dvalue = jnp.einsum('hbt,bhd->td', prob_low.astype(jnp.float32), o_blk).astype(jnp.bfloat16)
    return (dquery, dkey, dvalue)

def reference(queries, keys, values, out_grad, documents, query_weight, key_weight, value_weight):
    reps = N_SEQ // KV
    grads = []
    for section in range(SECTIONS):

        def one_slot(index):
            return slot_grads(index, queries[section], keys[section], values[section], out_grad[section], documents[section])
        dq_s, dk_s, dv_s = lax.map(one_slot, jnp.arange(N_SEQ, dtype=jnp.int32))
        total = queries.shape[1]
        dquery = jnp.transpose(dq_s, (1, 0, 2)).reshape(total, H * HD)
        dkey = jnp.transpose(dk_s, (1, 0, 2)).reshape(total, N_SEQ * HD)
        dvalue = jnp.transpose(dv_s, (1, 0, 2)).reshape(total, N_SEQ * HD)
        wk_rep = jnp.repeat(key_weight[section].reshape(KV, HD, D), reps, axis=0).reshape(N_SEQ * HD, D)
        wv_rep = jnp.repeat(value_weight[section].reshape(KV, HD, D), reps, axis=0).reshape(N_SEQ * HD, D)
        dinput = jnp.dot(dquery, query_weight[section], preferred_element_type=jnp.float32)
        dinput = dinput + jnp.dot(dkey, wk_rep, preferred_element_type=jnp.float32)
        dinput = dinput + jnp.dot(dvalue, wv_rep, preferred_element_type=jnp.float32)
        grads.append(dinput.astype(jnp.bfloat16))
    grads = grads[1:] + [jnp.zeros_like(grads[0])]
    return jnp.stack(grads, axis=0)
```

```python
import functools
import math

import jax
import jax.numpy as jnp
from jax import lax
from jax.experimental import pallas as pl
from jax.experimental.pallas import tpu as pltpu
from jax.sharding import PartitionSpec as P

HD = 128
MESH = pl.DeviceIdType.MESH
F32 = jnp.float32
BF16 = jnp.bfloat16


def aligned(index, size):
    return pl.ds(pl.multiple_of(index * size, size), size)


def kernel(dims, q_in, k_in, v_in, o_in, ids_ref, wq_in, wk_in, wv_in, out_ref,
           q_all, o_all, kv_all, k_turned, bias, dk_sum, dv_sum, dq_buf, grads, kv_grads,
           weights, kv_weights, right_buf, left_buf, acc, final,
           qo_sent, qo_got, kv_sent, kv_got, kv_passed, w_local, w_sent, w_got,
           dq_sent, g_got, kvg_sent, kvg_got,
           right_sent, right_got, left_sent, left_got, final_sent, final_got):
    sections, count, tok, heads, kv, width, cw, group, reach = dims
    chips = count // 2
    rows = 2 * tok
    feats = heads * HD
    chip_heads = 2 * heads
    own_heads = chips * heads
    half_feats = own_heads * HD
    kvh = kv // 2
    per = own_heads // kvh
    chunks = width // cw
    span = 2 * kvh * HD
    scale = 1.0 / math.sqrt(HD)
    to_log2 = scale * math.log2(math.e)
    sec = lax.axis_index("section")
    me = lax.axis_index("seq")
    chip = me // 2
    core = me % 2
    partner = (sec, me + 1 - 2 * core)
    last = chips - 1

    barrier = pltpu.get_barrier_semaphore()

    def greet(device):
        pl.semaphore_signal(barrier, inc=1, device_id=device, device_id_type=MESH)

    for off in range(1, count):
        greet((sec, lax.rem(me + off, count)))

    @pl.when(sec > 0)
    def _():
        greet((sec - 1, me))

    @pl.when(sec < sections - 1)
    def _():
        greet((sec + 1, me))

    above = jnp.where(sec > 0, 1, 0)
    below = jnp.where(sec < sections - 1, 1, 0)
    pl.semaphore_wait(barrier, count - 1 + above + below)

    def remote(src, dst, send_sem, recv_sem, device):
        return pltpu.make_async_remote_copy(
            src_ref=src, dst_ref=dst, send_sem=send_sem, recv_sem=recv_sem,
            device_id=device, device_id_type=MESH)

    kv_in = (k_in, v_in)
    right = jnp.minimum(chip + 1, last)

    def kv_head(half, g):
        return pl.ds(pl.multiple_of((half * kvh + g) * HD, HD), HD)

    def kv_right(which, g, p):
        return remote(kv_in[which].at[:, kv_head(p, g)],
                      kv_all.at[which, g, pl.ds(pl.multiple_of((reach - 1) * rows + core * tok, tok), tok)],
                      kv_sent.at[which, g, p], kv_got.at[which, g, 1, core], (sec, 2 * right + p))

    def kv_partner(which, g):
        return remote(kv_in[which].at[:, kv_head(1 - core, g)],
                      kv_all.at[which, g, pl.ds(pl.multiple_of(reach * rows + core * tok, tok), tok)],
                      kv_sent.at[which, g, 2], kv_got.at[which, g, 0, core], partner)

    def kv_own(which, g):
        return pltpu.make_async_copy(
            kv_in[which].at[:, kv_head(core, g)],
            kv_all.at[which, g, pl.ds(pl.multiple_of(reach * rows + core * tok, tok), tok)],
            kv_got.at[which, g, 0, core])

    def kv_block(which, g, e):
        return kv_all.at[which, g, pl.ds((reach - e) * rows, rows)]

    def kv_relay(which, g, e):
        return remote(kv_block(which, g, e), kv_block(which, g, e + 1),
                      kv_passed.at[which, g, e], kv_got.at[which, g, e + 1, 0],
                      (sec, 2 * right + core))

    def kv_wait(g, e):
        for which in range(2):
            if e < 2:
                for p in range(2):
                    part = kv_all.at[which, g, pl.ds((reach - e) * rows + p * tok, tok)]
                    pltpu.make_async_copy(part, part, kv_got.at[which, g, e, p]).wait()
            else:
                part = kv_block(which, g, e)
                pltpu.make_async_copy(part, part, kv_got.at[which, g, e, 0]).wait()

    def qo_partner(which):
        return remote((q_in, o_in)[which].at[:, aligned(1 - core, half_feats)],
                      (q_all, o_all)[which].at[aligned(core, tok)],
                      qo_sent.at[which], qo_got.at[which, 0], partner)

    def qo_own(which):
        return pltpu.make_async_copy((q_in, o_in)[which].at[:, aligned(core, half_feats)],
                                     (q_all, o_all)[which].at[aligned(core, tok)],
                                     qo_got.at[which, 1])

    w_copy = remote(wq_in, weights.at[aligned(core, feats)], w_sent.at[0], w_got.at[0], partner)

    @pl.when(chip < last)
    def _():
        for g in range(kvh):
            for which in range(2):
                for p in range(2):
                    kv_right(which, g, p).start()

    for g in range(kvh):
        for which in range(2):
            kv_own(which, g).start()
            kv_partner(which, g).start()
    for which in range(2):
        qo_own(which).start()
        qo_partner(which).start()

    w_copy.start()
    local = [pltpu.make_async_copy(wq_in, weights.at[aligned(core, feats)], w_local.at[0])]
    for r in range(2):
        part = slice(r * kvh * HD, (r + 1) * kvh * HD)
        for which, source in enumerate((wk_in, wv_in)):
            base = r * span + which * kvh * HD
            local.append(pltpu.make_async_copy(
                source.at[part], kv_weights.at[base:base + kvh * HD],
                w_local.at[1 + 2 * r + which]))
    for copy in local:
        copy.start()

    @pl.when(sec == sections - 1)
    def _():
        out_ref[...] = jnp.zeros_like(out_ref)

    q_ids = ids_ref[:, aligned(chip, rows)]

    def set_bias(blocks):
        here = blocks * rows
        first = pl.ds(pl.multiple_of((chip + 1 - blocks) * rows, rows), here)
        k_ids = jnp.broadcast_to(ids_ref[:, first], (HD, here)).T[:, :1]
        same = k_ids == q_ids
        j = lax.broadcasted_iota(jnp.int32, (here, rows), 0)
        i = lax.broadcasted_iota(jnp.int32, (here, rows), 1) + (blocks - 1) * rows
        bias[:here] = jnp.where(same & (j <= i), 0.0, -jnp.inf)

    for blocks in range(1, reach + 2):
        @pl.when(jnp.minimum(chip, reach) + 1 == blocks)
        def _():
            set_bias(blocks)

    for e in range(1, reach):
        @pl.when((chip >= e) & (chip < last))
        def _():
            for g in range(kvh):
                kv_wait(g, e)
                for which in range(2):
                    kv_relay(which, g, e).start()

    for which in range(2):
        buf = (q_all, o_all)[which]
        qo_own(which).wait()
        part = buf.at[aligned(1 - core, tok)]
        pltpu.make_async_copy(part, part, qo_got.at[which, 0]).wait()

    def dq_place(unit):
        head = unit * group
        target = core * (chips // 2) + head // chip_heads
        piece = (head % chip_heads) // group
        return target, piece

    def dq_copy(unit, p):
        target, piece = dq_place(unit)
        return remote(dq_buf.at[unit, p * tok:(p + 1) * tok],
                      grads.at[chip, :, aligned(piece, group * HD)],
                      dq_sent.at[unit, p], g_got.at[chip, piece], (sec, 2 * target + p))

    def dq_out(unit):
        target, piece = dq_place(unit)
        for p in range(2):
            @pl.when(2 * target + p != me)
            def _():
                dq_copy(unit, p).start()

            @pl.when(2 * target + p == me)
            def _():
                grads[chip, :, aligned(piece, group * HD)] = dq_buf[unit, p * tok:(p + 1) * tok]

    dims_last = (((1,), (1,)), ((), ()))

    def attend(blocks):
        here = blocks * rows
        low = (reach + 1 - blocks) * rows
        for g in range(kvh):
            for e in range(blocks):
                if 1 <= e < reach:
                    @pl.when(chip == last)
                    def _():
                        kv_wait(g, e)
                else:
                    kv_wait(g, e)
            k_turned[:, :here] = kv_all[0, g, low:].T
            dk_sum[:here] = jnp.zeros((here, HD), F32)
            dv_sum[:here] = jnp.zeros((here, HD), F32)

            def one_unit(n, carry):
                unit = g * (per // group) + n
                dk = jnp.zeros((here, HD), F32)
                dv = jnp.zeros((here, HD), F32)
                for h in range(group):
                    col = aligned(unit * group + h, HD)
                    q = q_all[:, col]
                    o = o_all[:, col]
                    s = lax.dot_general(kv_all[0, g, low:], q, dims_last, preferred_element_type=F32)
                    dp = lax.dot_general(kv_all[1, g, low:], o, dims_last, preferred_element_type=F32)
                    s = s + bias[:here]
                    top = jnp.max(s, axis=0, keepdims=True)
                    e = jnp.exp2((s - top) * to_log2)
                    inv = 1.0 / jnp.sum(e, axis=0, keepdims=True)
                    delta = jnp.sum(e * dp, axis=0, keepdims=True) * inv
                    prob = e * inv
                    ds = (prob * (dp - delta)).astype(BF16)
                    dv += jnp.dot(prob.astype(BF16), o, preferred_element_type=F32)
                    dk += jnp.dot(ds, q, preferred_element_type=F32)
                    dq = jnp.dot(k_turned[:, :here], ds, preferred_element_type=F32) * scale
                    dq_buf[unit, :, h * HD:(h + 1) * HD] = dq.T.astype(BF16)
                dk_sum[:here] += dk
                dv_sum[:here] += dv
                dq_out(unit)
                return carry

            lax.fori_loop(0, per // group, one_unit, 0)
            for e in range(blocks):
                at = (blocks - 1 - e) * rows
                for which, sums in enumerate((dk_sum, dv_sum)):
                    col = aligned(core * 2 * kvh + which * kvh + g, HD)
                    for p in range(2):
                        part = sums[at + p * tok:at + (p + 1) * tok]
                        if which == 0:
                            part = part * scale
                        kv_grads[e, p, :, col] = part.astype(BF16)

    def kvg_copy(e):
        part = kv_grads.at[e, 1 - core, :, aligned(core, span)]
        return remote(part, part, kvg_sent.at[e], kvg_got.at[e], partner)

    for blocks in range(1, reach + 2):
        @pl.when(jnp.minimum(chip, reach) + 1 == blocks)
        def _():
            attend(blocks)
            for e in range(blocks):
                kvg_copy(e).start()
            if blocks == 1:
                for copy in local:
                    copy.wait()
                part = weights.at[aligned(1 - core, feats)]
                pltpu.make_async_copy(part, part, w_got.at[0]).wait()
            else:
                for copy in local:
                    copy.wait()
                part = weights.at[aligned(1 - core, feats)]
                pltpu.make_async_copy(part, part, w_got.at[0]).wait()

    def kvg_wait(e):
        part = kv_grads.at[e, core, :, aligned(1 - core, span)]
        pltpu.make_async_copy(part, part, kvg_got.at[e]).wait()

    for e in range(reach + 1):
        @pl.when(chip >= e)
        def _():
            kvg_wait(e)

    def grads_wait(b):
        for piece in range(chip_heads // group):
            part = grads.at[b, :, piece * group * HD:(piece + 1) * group * HD]
            pltpu.make_async_copy(part, part, g_got.at[b, piece]).wait()

    for b in range(chips):
        @pl.when((chip == b) & (b // (chips // 2) != core))
        def _():
            grads_wait(b)

    def right_copy(d, k):
        here = right_buf.at[d, k]
        return remote(here, here, right_sent.at[d, k], right_got.at[d, k],
                      (sec, jnp.minimum(me + 2, count - 2 + core)))

    def left_copy(d, k):
        here = left_buf.at[d, k]
        return remote(here, here, left_sent.at[d, k], left_got.at[d, k],
                      (sec, jnp.maximum(me - 2, core)))

    def final_copy(k):
        return remote(final.at[k], out_ref.at[:, aligned(k, cw)], final_sent.at[k], final_got.at[k],
                      (jnp.maximum(sec - 1, 0), me))

    def product(d, k):
        acc[...] = jnp.dot(grads[d], weights[:, aligned(k, cw)], preferred_element_type=F32)

    def kv_product(e, k):
        acc[...] += jnp.dot(kv_grads[e, core], kv_weights[:, aligned(k, cw)],
                            preferred_element_type=F32)

    def pass_right(d, k):
        product(d, k)

        @pl.when(chip > 0)
        def _():
            right_copy(d, k).wait_recv()
            acc[...] += right_buf[d, k].astype(F32)

        right_buf[d, k] = acc[...].astype(BF16)
        right_copy(d, k).start()

    def pass_left(d, k):
        product(d, k)

        @pl.when(chip - d <= reach)
        def _():
            kv_product(jnp.minimum(chip - d, reach), k)

        @pl.when(chip < last)
        def _():
            left_copy(d, k).wait_recv()
            acc[...] += left_buf[d, k].astype(F32)

        left_buf[d, k] = acc[...].astype(BF16)
        left_copy(d, k).start()

    def finish(k):
        product(chip, k)
        kv_product(0, k)

        @pl.when(chip > 0)
        def _():
            right_copy(chip, k).wait_recv()
            acc[...] += right_buf[chip, k].astype(F32)

        @pl.when(chip < last)
        def _():
            left_copy(chip, k).wait_recv()
            acc[...] += left_buf[chip, k].astype(F32)

        final[k] = acc[...].astype(BF16)

        @pl.when(sec > 0)
        def _():
            final_copy(k).start()

    def each(first, end, act):
        def one(k, carry):
            act(k)
            return carry

        lax.fori_loop(first, end, one, 0)

    early = chunks * 3 // 8 if chips > 2 else 0

    if early:
        @pl.when(chip == 0)
        def _():
            grads_wait(1)
            each(0, early, lambda k: pass_right(1, k))

    for i in range(chips - 1):
        far, near = chips - 1 - i, i
        to_right = chip < far
        to_left = chip > near
        begin = early if i == chips - 2 else 0

        @pl.when(to_right)
        def _():
            if begin == 0:
                grads_wait(far)

        @pl.when(to_left)
        def _():
            grads_wait(near)

        def one(k):
            if begin == 0:
                @pl.when(to_right)
                def _():
                    pass_right(far, k)
            else:
                @pl.when(to_right & (k >= begin))
                def _():
                    pass_right(far, k)

            @pl.when(to_left)
            def _():
                pass_left(near, k)

            if i == 1 and early:
                @pl.when((chip == 1) & (k < early))
                def _():
                    finish(k)

        each(0, chunks, one)

    each(0, early, lambda k: pl.when(chip != 1)(lambda: finish(k)))
    each(early, chunks, finish)

    @pl.when(chip < last)
    def _():
        for g in range(kvh):
            for which in range(2):
                for p in range(2):
                    kv_right(which, g, p).wait_send()

    for e in range(1, reach):
        @pl.when((chip >= e) & (chip < last))
        def _():
            for g in range(kvh):
                for which in range(2):
                    kv_relay(which, g, e).wait_send()

    for which in range(2):
        for g in range(kvh):
            kv_partner(which, g).wait_send()
        qo_partner(which).wait_send()
    w_copy.wait_send()

    def dq_done(unit, carry):
        target, _ = dq_place(unit)
        for p in range(2):
            @pl.when(2 * target + p != me)
            def _():
                dq_copy(unit, p).wait_send()
        return carry

    lax.fori_loop(0, own_heads // group, dq_done, 0)

    for e in range(reach + 1):
        @pl.when(chip >= e)
        def _():
            kvg_copy(e).wait_send()

    def drain(k):
        def right_done(i, c):
            right_copy(last - i, k).wait_send()
            return c

        def left_done(i, c):
            left_copy(i, k).wait_send()
            return c

        lax.fori_loop(0, last - chip, right_done, 0)
        lax.fori_loop(0, chip, left_done, 0)

        @pl.when(sec > 0)
        def _():
            final_copy(k).wait_send()

        @pl.when(sec < sections - 1)
        def _():
            final_copy(k).wait_recv()

    each(0, chunks, drain)


def body(queries, keys, values, out_grad, documents, query_weight, key_weight, value_weight):
    sections = lax.axis_size("section")
    count = lax.axis_size("seq")
    tok = queries.shape[1]
    total = tok * count
    kv = keys.shape[2] // HD
    feats = query_weight.shape[1]
    heads = feats // HD
    width = query_weight.shape[2]
    chips = count // 2
    rows = 2 * tok
    reach = -(-(total // 2) // rows)
    group = 2
    cw = min(512, width)
    chunks = width // cw
    units = chips * heads // group
    kvh = kv // 2
    slots = (reach + 1) * rows
    dma = pltpu.SemaphoreType.DMA
    anywhere = pl.BlockSpec(memory_space=pl.ANY)
    vmem = pl.BlockSpec(memory_space=pltpu.VMEM)
    out = pl.pallas_call(
        functools.partial(kernel, (sections, count, tok, heads, kv, width, cw, group, reach)),
        out_shape=jax.ShapeDtypeStruct((tok, width), BF16),
        in_specs=[anywhere] * 4 + [vmem] + [anywhere] * 3,
        out_specs=vmem,
        scratch_shapes=[
            pltpu.VMEM((rows, chips * feats), BF16),
            pltpu.VMEM((rows, chips * feats), BF16),
            pltpu.VMEM((2, kvh, slots, HD), BF16),
            pltpu.VMEM((HD, slots), BF16),
            pltpu.VMEM((slots, rows), F32),
            pltpu.VMEM((slots, HD), F32),
            pltpu.VMEM((slots, HD), F32),
            pltpu.VMEM((units, rows, group * HD), BF16),
            pltpu.VMEM((chips, tok, 2 * feats), BF16),
            pltpu.VMEM((reach + 1, 2, tok, 2 * kv * HD), BF16),
            pltpu.VMEM((2 * feats, width), BF16),
            pltpu.VMEM((2 * kv * HD, width), BF16),
            pltpu.VMEM((chips, chunks, tok, cw), BF16),
            pltpu.VMEM((chips, chunks, tok, cw), BF16),
            pltpu.VMEM((tok, cw), F32),
            pltpu.VMEM((chunks, tok, cw), BF16),
            dma((2,)),
            dma((2, 2)),
            dma((2, kvh, 3)),
            dma((2, kvh, reach + 1, 2)),
            dma((2, kvh, reach + 1)),
            dma((5,)),
            dma((1,)),
            dma((1,)),
            dma((units, 2)),
            dma((chips, 2 * heads // group)),
            dma((reach + 1,)),
            dma((reach + 1,)),
            dma((chips, chunks)),
            dma((chips, chunks)),
            dma((chips, chunks)),
            dma((chips, chunks)),
            dma((chunks,)),
            dma((chunks,)),
        ],
        compiler_params=pltpu.CompilerParams(
            collective_id=0, has_side_effects=True, vmem_limit_bytes=62 * 1024 * 1024),
        name="attention_back",
    )(queries[0], keys[0], values[0], out_grad[0], documents,
      query_weight[0], key_weight[0], value_weight[0])
    return out[None]


def solution(mesh):
    in_specs = (
        P("section", "seq", None),
        P("section", "seq", None),
        P("section", "seq", None),
        P("section", "seq", None),
        P("section", None),
        P("section", "seq", None),
        P("section", None, None),
        P("section", None, None),
    )
    out_specs = P("section", "seq", None)
    return jax.shard_map(body, mesh=mesh, in_specs=in_specs, out_specs=out_specs, check_vma=False)
```

```python
import functools
import math

import jax
import jax.numpy as jnp
from jax import lax
from jax.experimental import pallas as pl
from jax.experimental.pallas import tpu as pltpu
from jax.sharding import PartitionSpec as P

HD = 128
MESH = pl.DeviceIdType.MESH
F32 = jnp.float32
BF16 = jnp.bfloat16


def aligned(index, size):
    return pl.ds(pl.multiple_of(index * size, size), size)


def kernel(dims, q_in, k_in, v_in, o_in, ids_ref, wq_in, wk_in, wv_in, out_ref,
           q_all, o_all, kv_all, k_turned, bias, dk_sum, dv_sum, dq_buf, grads, kv_grads,
           weights, kv_weights, right_buf, left_buf, acc, final,
           qo_sent, qo_got, kv_sent, kv_got, kv_passed, w_local, w_sent, w_got,
           dq_sent, g_got, kvg_sent, kvg_got,
           right_sent, right_got, left_sent, left_got, final_sent, final_got):
    sections, count, tok, heads, kv, width, cw, group, reach = dims
    chips = count // 2
    rows = 2 * tok
    feats = heads * HD
    chip_heads = 2 * heads
    own_heads = chips * heads
    half_feats = own_heads * HD
    kvh = kv // 2
    per = own_heads // kvh
    chunks = width // cw
    span = 2 * kvh * HD
    scale = 1.0 / math.sqrt(HD)
    to_log2 = scale * math.log2(math.e)
    sec = lax.axis_index("section")
    me = lax.axis_index("seq")
    chip = me // 2
    core = me % 2
    partner = (sec, me + 1 - 2 * core)
    last = chips - 1

    barrier = pltpu.get_barrier_semaphore()

    def greet(device):
        pl.semaphore_signal(barrier, inc=1, device_id=device, device_id_type=MESH)

    for off in range(1, count):
        greet((sec, lax.rem(me + off, count)))

    @pl.when(sec > 0)
    def _():
        greet((sec - 1, me))

    @pl.when(sec < sections - 1)
    def _():
        greet((sec + 1, me))

    above = jnp.where(sec > 0, 1, 0)
    below = jnp.where(sec < sections - 1, 1, 0)
    with jax.named_scope('barrier'):
        pl.semaphore_wait(barrier, count - 1 + above + below)

    def remote(src, dst, send_sem, recv_sem, device):
        return pltpu.make_async_remote_copy(
            src_ref=src, dst_ref=dst, send_sem=send_sem, recv_sem=recv_sem,
            device_id=device, device_id_type=MESH)

    kv_in = (k_in, v_in)
    right = jnp.minimum(chip + 1, last)

    def kv_head(half, g):
        return pl.ds(pl.multiple_of((half * kvh + g) * HD, HD), HD)

    def kv_right(which, g, p):
        return remote(kv_in[which].at[:, kv_head(p, g)],
                      kv_all.at[which, g, pl.ds(pl.multiple_of((reach - 1) * rows + core * tok, tok), tok)],
                      kv_sent.at[which, g, p], kv_got.at[which, g, 1, core], (sec, 2 * right + p))

    def kv_partner(which, g):
        return remote(kv_in[which].at[:, kv_head(1 - core, g)],
                      kv_all.at[which, g, pl.ds(pl.multiple_of(reach * rows + core * tok, tok), tok)],
                      kv_sent.at[which, g, 2], kv_got.at[which, g, 0, core], partner)

    def kv_own(which, g):
        return pltpu.make_async_copy(
            kv_in[which].at[:, kv_head(core, g)],
            kv_all.at[which, g, pl.ds(pl.multiple_of(reach * rows + core * tok, tok), tok)],
            kv_got.at[which, g, 0, core])

    def kv_block(which, g, e):
        return kv_all.at[which, g, pl.ds((reach - e) * rows, rows)]

    def kv_relay(which, g, e):
        return remote(kv_block(which, g, e), kv_block(which, g, e + 1),
                      kv_passed.at[which, g, e], kv_got.at[which, g, e + 1, 0],
                      (sec, 2 * right + core))

    def kv_wait(g, e):
        for which in range(2):
            if e < 2:
                for p in range(2):
                    part = kv_all.at[which, g, pl.ds((reach - e) * rows + p * tok, tok)]
                    pltpu.make_async_copy(part, part, kv_got.at[which, g, e, p]).wait()
            else:
                part = kv_block(which, g, e)
                pltpu.make_async_copy(part, part, kv_got.at[which, g, e, 0]).wait()

    def qo_partner(which):
        return remote((q_in, o_in)[which].at[:, aligned(1 - core, half_feats)],
                      (q_all, o_all)[which].at[aligned(core, tok)],
                      qo_sent.at[which], qo_got.at[which, 0], partner)

    def qo_own(which):
        return pltpu.make_async_copy((q_in, o_in)[which].at[:, aligned(core, half_feats)],
                                     (q_all, o_all)[which].at[aligned(core, tok)],
                                     qo_got.at[which, 1])

    w_copy = remote(wq_in, weights.at[aligned(core, feats)], w_sent.at[0], w_got.at[0], partner)

    @pl.when(chip < last)
    def _():
        for g in range(kvh):
            for which in range(2):
                for p in range(2):
                    kv_right(which, g, p).start()

    for g in range(kvh):
        for which in range(2):
            kv_own(which, g).start()
            kv_partner(which, g).start()
    for which in range(2):
        qo_own(which).start()
        qo_partner(which).start()

    w_copy.start()
    local = [pltpu.make_async_copy(wq_in, weights.at[aligned(core, feats)], w_local.at[0])]
    for r in range(2):
        part = slice(r * kvh * HD, (r + 1) * kvh * HD)
        for which, source in enumerate((wk_in, wv_in)):
            base = r * span + which * kvh * HD
            local.append(pltpu.make_async_copy(
                source.at[part], kv_weights.at[base:base + kvh * HD],
                w_local.at[1 + 2 * r + which]))
    for copy in local:
        copy.start()

    @pl.when(sec == sections - 1)
    def _():
        out_ref[...] = jnp.zeros_like(out_ref)

    q_ids = ids_ref[:, aligned(chip, rows)]

    def set_bias(blocks):
        here = blocks * rows
        first = pl.ds(pl.multiple_of((chip + 1 - blocks) * rows, rows), here)
        k_ids = jnp.broadcast_to(ids_ref[:, first], (HD, here)).T[:, :1]
        same = k_ids == q_ids
        j = lax.broadcasted_iota(jnp.int32, (here, rows), 0)
        i = lax.broadcasted_iota(jnp.int32, (here, rows), 1) + (blocks - 1) * rows
        bias[:here] = jnp.where(same & (j <= i), 0.0, -jnp.inf)

    for blocks in range(1, reach + 2):
        @pl.when(jnp.minimum(chip, reach) + 1 == blocks)
        def _():
            with jax.named_scope('bias'):
                set_bias(blocks)

    for e in range(1, reach):
        @pl.when((chip >= e) & (chip < last))
        def _():
            with jax.named_scope('relay'):
                for g in range(kvh):
                    kv_wait(g, e)
                    for which in range(2):
                        kv_relay(which, g, e).start()

    with jax.named_scope('qo_wait'):
        for which in range(2):
            buf = (q_all, o_all)[which]
            qo_own(which).wait()
            part = buf.at[aligned(1 - core, tok)]
            pltpu.make_async_copy(part, part, qo_got.at[which, 0]).wait()

    def dq_place(unit):
        head = unit * group
        target = core * (chips // 2) + head // chip_heads
        piece = (head % chip_heads) // group
        return target, piece

    def dq_copy(unit, p):
        target, piece = dq_place(unit)
        return remote(dq_buf.at[unit, p * tok:(p + 1) * tok],
                      grads.at[chip, :, aligned(piece, group * HD)],
                      dq_sent.at[unit, p], g_got.at[chip, piece], (sec, 2 * target + p))

    def dq_out(unit):
        target, piece = dq_place(unit)
        for p in range(2):
            @pl.when(2 * target + p != me)
            def _():
                dq_copy(unit, p).start()

            @pl.when(2 * target + p == me)
            def _():
                grads[chip, :, aligned(piece, group * HD)] = dq_buf[unit, p * tok:(p + 1) * tok]

    dims_last = (((1,), (1,)), ((), ()))

    def attend(blocks):
        here = blocks * rows
        low = (reach + 1 - blocks) * rows
        for g in range(kvh):
            with jax.named_scope('kv_wait'):
                for e in range(blocks):
                    if 1 <= e < reach:
                        @pl.when(chip == last)
                        def _():
                            kv_wait(g, e)
                    else:
                        kv_wait(g, e)
            k_turned[:, :here] = kv_all[0, g, low:].T
            dk_sum[:here] = jnp.zeros((here, HD), F32)
            dv_sum[:here] = jnp.zeros((here, HD), F32)

            def one_unit(n, carry):
                unit = g * (per // group) + n
                dk = jnp.zeros((here, HD), F32)
                dv = jnp.zeros((here, HD), F32)
                for h in range(group):
                    col = aligned(unit * group + h, HD)
                    q = q_all[:, col]
                    o = o_all[:, col]
                    s = lax.dot_general(kv_all[0, g, low:], q, dims_last, preferred_element_type=F32)
                    dp = lax.dot_general(kv_all[1, g, low:], o, dims_last, preferred_element_type=F32)
                    s = s + bias[:here]
                    top = jnp.max(s, axis=0, keepdims=True)
                    e = jnp.exp2((s - top) * to_log2)
                    inv = 1.0 / jnp.sum(e, axis=0, keepdims=True)
                    delta = jnp.sum(e * dp, axis=0, keepdims=True) * inv
                    prob = e * inv
                    ds = (prob * (dp - delta)).astype(BF16)
                    dv += jnp.dot(prob.astype(BF16), o, preferred_element_type=F32)
                    dk += jnp.dot(ds, q, preferred_element_type=F32)
                    dq = jnp.dot(k_turned[:, :here], ds, preferred_element_type=F32) * scale
                    dq_buf[unit, :, h * HD:(h + 1) * HD] = dq.T.astype(BF16)
                dk_sum[:here] += dk
                dv_sum[:here] += dv
                dq_out(unit)
                return carry

            with jax.named_scope('attend'):
                lax.fori_loop(0, per // group, one_unit, 0)
            for e in range(blocks):
                at = (blocks - 1 - e) * rows
                for which, sums in enumerate((dk_sum, dv_sum)):
                    col = aligned(core * 2 * kvh + which * kvh + g, HD)
                    for p in range(2):
                        part = sums[at + p * tok:at + (p + 1) * tok]
                        if which == 0:
                            part = part * scale
                        kv_grads[e, p, :, col] = part.astype(BF16)

    def kvg_copy(e):
        part = kv_grads.at[e, 1 - core, :, aligned(core, span)]
        return remote(part, part, kvg_sent.at[e], kvg_got.at[e], partner)

    for blocks in range(1, reach + 2):
        @pl.when(jnp.minimum(chip, reach) + 1 == blocks)
        def _():
            attend(blocks)
            for e in range(blocks):
                kvg_copy(e).start()

    def kvg_wait(e):
        part = kv_grads.at[e, core, :, aligned(1 - core, span)]
        pltpu.make_async_copy(part, part, kvg_got.at[e]).wait()

    with jax.named_scope('w_wait'):
        for copy in local:
            copy.wait()
        theirs = weights.at[aligned(1 - core, feats)]
        pltpu.make_async_copy(theirs, theirs, w_got.at[0]).wait()

    with jax.named_scope('kvg_wait'):
        for e in range(reach + 1):
            @pl.when(chip >= e)
            def _():
                kvg_wait(e)

    def grads_wait(b):
        with jax.named_scope('g_wait'):
            for piece in range(chip_heads // group):
                part = grads.at[b, :, piece * group * HD:(piece + 1) * group * HD]
                pltpu.make_async_copy(part, part, g_got.at[b, piece]).wait()

    for b in range(chips):
        @pl.when((chip == b) & (b // (chips // 2) != core))
        def _():
            grads_wait(b)

    def right_copy(d, k):
        here = right_buf.at[d, k]
        return remote(here, here, right_sent.at[d, k], right_got.at[d, k],
                      (sec, jnp.minimum(me + 2, count - 2 + core)))

    def left_copy(d, k):
        here = left_buf.at[d, k]
        return remote(here, here, left_sent.at[d, k], left_got.at[d, k],
                      (sec, jnp.maximum(me - 2, core)))

    def final_copy(k):
        return remote(final.at[k], out_ref.at[:, aligned(k, cw)], final_sent.at[k], final_got.at[k],
                      (jnp.maximum(sec - 1, 0), me))

    def product(d, k):
        acc[...] = jnp.dot(grads[d], weights[:, aligned(k, cw)], preferred_element_type=F32)

    def kv_product(e, k):
        acc[...] += jnp.dot(kv_grads[e, core], kv_weights[:, aligned(k, cw)],
                            preferred_element_type=F32)

    def pass_right(d, k):
        with jax.named_scope('r_prod'):
            product(d, k)

        @pl.when(chip > 0)
        def _():
            with jax.named_scope('r_wait'):
                right_copy(d, k).wait_recv()
            acc[...] += right_buf[d, k].astype(F32)

        right_buf[d, k] = acc[...].astype(BF16)
        right_copy(d, k).start()

    def pass_left(d, k):
        with jax.named_scope('l_prod'):
            product(d, k)

            @pl.when(chip - d <= reach)
            def _():
                kv_product(jnp.minimum(chip - d, reach), k)

        @pl.when(chip < last)
        def _():
            with jax.named_scope('l_wait'):
                left_copy(d, k).wait_recv()
            acc[...] += left_buf[d, k].astype(F32)

        left_buf[d, k] = acc[...].astype(BF16)
        left_copy(d, k).start()

    def finish(k):
        with jax.named_scope('f_prod'):
            product(chip, k)
            kv_product(0, k)

        @pl.when(chip > 0)
        def _():
            with jax.named_scope('f_wait_r'):
                right_copy(chip, k).wait_recv()
            acc[...] += right_buf[chip, k].astype(F32)

        @pl.when(chip < last)
        def _():
            with jax.named_scope('f_wait_l'):
                left_copy(chip, k).wait_recv()
            acc[...] += left_buf[chip, k].astype(F32)

        final[k] = acc[...].astype(BF16)

        @pl.when(sec > 0)
        def _():
            final_copy(k).start()

    def each(first, end, act):
        def one(k, carry):
            act(k)
            return carry

        lax.fori_loop(first, end, one, 0)

    early = chunks * 3 // 8 if chips > 2 else 0
    lag = 3
    leads_right = chip < chips // 2

    if early:
        @pl.when(chip == 0)
        def _():
            grads_wait(1)
            each(0, early, lambda k: pass_right(1, k))

    for i in range(chips - 1):
        far, near = chips - 1 - i, i
        to_right = chip < far
        to_left = chip > near
        begin = early if i == chips - 2 else 0

        @pl.when(to_right)
        def _():
            if begin == 0:
                grads_wait(far)

        @pl.when(to_left)
        def _():
            grads_wait(near)

        def one(step):
            k_right = step - jnp.where(leads_right, 0, lag)
            k_left = step - jnp.where(leads_right, lag, 0)

            @pl.when(to_right & (k_right >= begin) & (k_right < chunks))
            def _():
                pass_right(far, k_right)

            @pl.when(to_left & (k_left >= 0) & (k_left < chunks))
            def _():
                pass_left(near, k_left)

            if i == 1 and early:
                @pl.when((chip == 1) & (k_left >= 0) & (k_left < early))
                def _():
                    finish(k_left)

        each(0, chunks + lag, one)

    each(0, early, lambda k: pl.when(chip != 1)(lambda: finish(k)))
    each(early, chunks, finish)

    @pl.when(chip < last)
    def _():
        for g in range(kvh):
            for which in range(2):
                for p in range(2):
                    kv_right(which, g, p).wait_send()

    for e in range(1, reach):
        @pl.when((chip >= e) & (chip < last))
        def _():
            for g in range(kvh):
                for which in range(2):
                    kv_relay(which, g, e).wait_send()

    for which in range(2):
        for g in range(kvh):
            kv_partner(which, g).wait_send()
        qo_partner(which).wait_send()
    w_copy.wait_send()

    def dq_done(unit, carry):
        target, _ = dq_place(unit)
        for p in range(2):
            @pl.when(2 * target + p != me)
            def _():
                dq_copy(unit, p).wait_send()
        return carry

    lax.fori_loop(0, own_heads // group, dq_done, 0)

    for e in range(reach + 1):
        @pl.when(chip >= e)
        def _():
            kvg_copy(e).wait_send()

    def drain(k):
        def right_done(i, c):
            right_copy(last - i, k).wait_send()
            return c

        def left_done(i, c):
            left_copy(i, k).wait_send()
            return c

        lax.fori_loop(0, last - chip, right_done, 0)
        lax.fori_loop(0, chip, left_done, 0)

        @pl.when(sec > 0)
        def _():
            final_copy(k).wait_send()

        @pl.when(sec < sections - 1)
        def _():
            final_copy(k).wait_recv()

    with jax.named_scope('drain'):
        each(0, chunks, drain)


def body(queries, keys, values, out_grad, documents, query_weight, key_weight, value_weight):
    sections = lax.axis_size("section")
    count = lax.axis_size("seq")
    tok = queries.shape[1]
    total = tok * count
    kv = keys.shape[2] // HD
    feats = query_weight.shape[1]
    heads = feats // HD
    width = query_weight.shape[2]
    chips = count // 2
    rows = 2 * tok
    reach = -(-(total // 2) // rows)
    group = 2
    cw = min(512, width)
    chunks = width // cw
    units = chips * heads // group
    kvh = kv // 2
    slots = (reach + 1) * rows
    dma = pltpu.SemaphoreType.DMA
    anywhere = pl.BlockSpec(memory_space=pl.ANY)
    vmem = pl.BlockSpec(memory_space=pltpu.VMEM)
    out = pl.pallas_call(
        functools.partial(kernel, (sections, count, tok, heads, kv, width, cw, group, reach)),
        out_shape=jax.ShapeDtypeStruct((tok, width), BF16),
        in_specs=[anywhere] * 4 + [vmem] + [anywhere] * 3,
        out_specs=vmem,
        scratch_shapes=[
            pltpu.VMEM((rows, chips * feats), BF16),
            pltpu.VMEM((rows, chips * feats), BF16),
            pltpu.VMEM((2, kvh, slots, HD), BF16),
            pltpu.VMEM((HD, slots), BF16),
            pltpu.VMEM((slots, rows), F32),
            pltpu.VMEM((slots, HD), F32),
            pltpu.VMEM((slots, HD), F32),
            pltpu.VMEM((units, rows, group * HD), BF16),
            pltpu.VMEM((chips, tok, 2 * feats), BF16),
            pltpu.VMEM((reach + 1, 2, tok, 2 * kv * HD), BF16),
            pltpu.VMEM((2 * feats, width), BF16),
            pltpu.VMEM((2 * kv * HD, width), BF16),
            pltpu.VMEM((chips, chunks, tok, cw), BF16),
            pltpu.VMEM((chips, chunks, tok, cw), BF16),
            pltpu.VMEM((tok, cw), F32),
            pltpu.VMEM((chunks, tok, cw), BF16),
            dma((2,)),
            dma((2, 2)),
            dma((2, kvh, 3)),
            dma((2, kvh, reach + 1, 2)),
            dma((2, kvh, reach + 1)),
            dma((5,)),
            dma((1,)),
            dma((1,)),
            dma((units, 2)),
            dma((chips, 2 * heads // group)),
            dma((reach + 1,)),
            dma((reach + 1,)),
            dma((chips, chunks)),
            dma((chips, chunks)),
            dma((chips, chunks)),
            dma((chips, chunks)),
            dma((chunks,)),
            dma((chunks,)),
        ],
        compiler_params=pltpu.CompilerParams(
            collective_id=0, has_side_effects=True, vmem_limit_bytes=62 * 1024 * 1024),
        name="attention_back",
    )(queries[0], keys[0], values[0], out_grad[0], documents,
      query_weight[0], key_weight[0], value_weight[0])
    return out[None]


def solution(mesh):
    in_specs = (
        P("section", "seq", None),
        P("section", "seq", None),
        P("section", "seq", None),
        P("section", "seq", None),
        P("section", None),
        P("section", "seq", None),
        P("section", None, None),
        P("section", None, None),
    )
    out_specs = P("section", "seq", None)
    return jax.shard_map(body, mesh=mesh, in_specs=in_specs, out_specs=out_specs, check_vma=False)
```

```python
import functools
import math

import jax
import jax.numpy as jnp
from jax import lax
from jax.experimental import pallas as pl
from jax.experimental.pallas import tpu as pltpu
from jax.sharding import PartitionSpec as P

HD = 128
MESH = pl.DeviceIdType.MESH
F32 = jnp.float32
BF16 = jnp.bfloat16


def aligned(index, size):
    return pl.ds(pl.multiple_of(index * size, size), size)


def kernel(dims, q_in, k_in, v_in, o_in, ids_ref, wq_in, wk_in, wv_in, out_ref,
           q_all, o_all, kv_all, k_turned, bias, dk_sum, dv_sum, dq_buf, grads, kv_grads,
           weights, kv_weights, right_buf, left_buf, acc, final,
           qo_sent, qo_got, kv_sent, kv_got, kv_passed, w_local, w_sent, w_got,
           dq_sent, g_got, kvg_sent, kvg_got,
           right_sent, right_got, left_sent, left_got, final_sent, final_got):
    sections, count, tok, heads, kv, width, cw, group, reach = dims
    chips = count // 2
    rows = 2 * tok
    feats = heads * HD
    chip_heads = 2 * heads
    own_heads = chips * heads
    units = own_heads // group
    half_feats = own_heads * HD
    kvh = kv // 2
    per = own_heads // kvh
    chunks = width // cw
    span = 2 * kvh * HD
    scale = 1.0 / math.sqrt(HD)
    to_log2 = scale * math.log2(math.e)
    sec = lax.axis_index("section")
    me = lax.axis_index("seq")
    chip = me // 2
    core = me % 2
    partner = (sec, me + 1 - 2 * core)
    last = chips - 1

    barrier = pltpu.get_barrier_semaphore()

    def greet(device):
        pl.semaphore_signal(barrier, inc=1, device_id=device, device_id_type=MESH)

    for off in range(1, count):
        greet((sec, lax.rem(me + off, count)))

    @pl.when(sec > 0)
    def _():
        greet((sec - 1, me))

    @pl.when(sec < sections - 1)
    def _():
        greet((sec + 1, me))

    above = jnp.where(sec > 0, 1, 0)
    below = jnp.where(sec < sections - 1, 1, 0)
    with jax.named_scope('barrier'):
        pl.semaphore_wait(barrier, count - 1 + above + below)

    def remote(src, dst, send_sem, recv_sem, device):
        return pltpu.make_async_remote_copy(
            src_ref=src, dst_ref=dst, send_sem=send_sem, recv_sem=recv_sem,
            device_id=device, device_id_type=MESH)

    kv_in = (k_in, v_in)
    right = jnp.minimum(chip + 1, last)

    def kv_head(half, g):
        return pl.ds(pl.multiple_of((half * kvh + g) * HD, HD), HD)

    def kv_right(which, g, p):
        return remote(kv_in[which].at[:, kv_head(p, g)],
                      kv_all.at[which, g, pl.ds(pl.multiple_of((reach - 1) * rows + core * tok, tok), tok)],
                      kv_sent.at[0], kv_got.at[which, g, 1], (sec, 2 * right + p))

    def kv_direct(which, g, p):
        return remote(kv_in[which].at[:, kv_head(p, g)],
                      kv_all.at[which, g, pl.ds(pl.multiple_of((reach - 2) * rows + core * tok, tok), tok)],
                      kv_sent.at[0], kv_got.at[which, g, 2], (sec, 2 * last + p))

    def kv_partner(which, g):
        return remote(kv_in[which].at[:, kv_head(1 - core, g)],
                      kv_all.at[which, g, pl.ds(pl.multiple_of(reach * rows + core * tok, tok), tok)],
                      kv_sent.at[0], kv_got.at[which, g, 0], partner)

    def kv_own(which, g):
        return pltpu.make_async_copy(
            kv_in[which].at[:, kv_head(core, g)],
            kv_all.at[which, g, pl.ds(pl.multiple_of(reach * rows + core * tok, tok), tok)],
            kv_got.at[which, g, 0])

    def kv_block(which, g, e):
        return kv_all.at[which, g, pl.ds((reach - e) * rows, rows)]

    def kv_relay(which, g, e):
        return remote(kv_block(which, g, e), kv_block(which, g, e + 1),
                      kv_passed.at[0], kv_got.at[which, g, e + 1],
                      (sec, 2 * right + core))

    def kv_wait(which, g, e):
        part = kv_block(which, g, e)
        pltpu.make_async_copy(part, part, kv_got.at[which, g, e]).wait()

    def pass_kv(g, e):
        with jax.named_scope('relay'):
            for which in range(2):
                kv_wait(which, g, e)
                kv_relay(which, g, e).start()

    def qo_partner(which):
        return remote((q_in, o_in)[which].at[:, aligned(1 - core, half_feats)],
                      (q_all, o_all)[which].at[aligned(core, tok)],
                      qo_sent.at[which], qo_got.at[which, 0], partner)

    def qo_own(which):
        return pltpu.make_async_copy((q_in, o_in)[which].at[:, aligned(core, half_feats)],
                                     (q_all, o_all)[which].at[aligned(core, tok)],
                                     qo_got.at[which, 1])

    w_copy = remote(wq_in, weights.at[aligned(core, feats)], w_sent.at[0], w_got.at[0], partner)

    direct = reach > 1 and chips > 2

    def goes_on(g, e):
        return chip < (last - 1 if direct and g == 0 and e == 1 else last)

    def send_right(g):
        if direct and g == 0:
            @pl.when(chip == last - 2)
            def _():
                for which in range(2):
                    for p in range(2):
                        kv_direct(which, g, p).start()

        @pl.when(chip < last)
        def _():
            for which in range(2):
                for p in range(2):
                    kv_right(which, g, p).start()

    send_right(0)
    for g in range(1, kvh):
        send_right(g)

    for g in range(kvh):
        for which in range(2):
            kv_own(which, g).start()
            kv_partner(which, g).start()
    for which in range(2):
        qo_own(which).start()
        qo_partner(which).start()

    w_copy.start()
    local = [pltpu.make_async_copy(wq_in, weights.at[aligned(core, feats)], w_local.at[0])]
    for r in range(2):
        part = slice(r * kvh * HD, (r + 1) * kvh * HD)
        for which, source in enumerate((wk_in, wv_in)):
            base = r * span + which * kvh * HD
            local.append(pltpu.make_async_copy(
                source.at[part], kv_weights.at[base:base + kvh * HD],
                w_local.at[1 + 2 * r + which]))
    for copy in local:
        copy.start()

    @pl.when(sec == sections - 1)
    def _():
        out_ref[...] = jnp.zeros_like(out_ref)

    q_ids = ids_ref[:, aligned(chip, rows)]

    def set_bias(blocks):
        here = blocks * rows
        first = pl.ds(pl.multiple_of((chip + 1 - blocks) * rows, rows), here)
        k_ids = jnp.broadcast_to(ids_ref[:, first], (HD, here)).T[:, :1]
        same = k_ids == q_ids
        j = lax.broadcasted_iota(jnp.int32, (here, rows), 0)
        i = lax.broadcasted_iota(jnp.int32, (here, rows), 1) + (blocks - 1) * rows
        bias[:here] = jnp.where(same & (j <= i), 0.0, -jnp.inf)

    for blocks in range(1, reach + 2):
        @pl.when(jnp.minimum(chip, reach) + 1 == blocks)
        def _():
            with jax.named_scope('bias'):
                set_bias(blocks)

    for g in range(kvh):
        for e in range(1, reach):
            from_chip = e if g == 0 else max(e, 2)

            @pl.when((chip >= from_chip) & goes_on(g, e))
            def _():
                pass_kv(g, e)

    with jax.named_scope('qo_wait'):
        for which in range(2):
            buf = (q_all, o_all)[which]
            qo_own(which).wait()
            part = buf.at[aligned(1 - core, tok)]
            pltpu.make_async_copy(part, part, qo_got.at[which, 0]).wait()

    def dq_place(unit):
        head = unit * group
        target = core * (chips // 2) + head // chip_heads
        piece = (head % chip_heads) // group
        return target, piece

    def dq_copy(unit, p):
        target, piece = dq_place(unit)
        return remote(dq_buf.at[unit, p * tok:(p + 1) * tok],
                      grads.at[chip, :, aligned(piece, group * HD)],
                      dq_sent.at[0], g_got.at[chip], (sec, 2 * target + p))

    def dq_out(unit, reaches=None):
        target, piece = dq_place(unit)
        for p in range(2):
            @pl.when((2 * target + p != me) if reaches is None else (2 * target + p != me) & (target <= reaches))
            def _():
                dq_copy(unit, p).start()

            @pl.when(2 * target + p == me)
            def _():
                grads[chip, :, aligned(piece, group * HD)] = dq_buf[unit, p * tok:(p + 1) * tok]

    dims_last = (((1,), (1,)), ((), ()))

    early = chunks * 3 // 8 if chips > 2 else 0

    def far_out(first, end=chips):
        def far_unit(n, carry):
            unit = units - 1 - n
            target, _ = dq_place(unit)

            @pl.when((target >= first) & (target < end))
            def _():
                for p in range(2):
                    dq_copy(unit, p).start()

            return carry

        lax.fori_loop(0, units, far_unit, 0)

    held = min(2, reach)

    def attend(blocks):
        here = blocks * rows
        low = (reach + 1 - blocks) * rows
        for turn in range(kvh):
            g = jnp.where(core == 0, kvh - 1 - turn, turn) if blocks == 1 else turn
            with jax.named_scope('kv_wait'):
                for e in range(blocks):
                    if 1 <= e < reach:
                        @pl.when(~goes_on(g, e))
                        def _():
                            kv_wait(0, g, e)
                            kv_wait(1, g, e)
                    else:
                        kv_wait(0, g, e)
                        kv_wait(1, g, e)
            k_turned[:, :here] = kv_all[0, g, low:].T
            dk_sum[:here] = jnp.zeros((here, HD), F32)
            dv_sum[:here] = jnp.zeros((here, HD), F32)

            def one_unit(n, carry):
                unit = g * (per // group) + n
                dk = jnp.zeros((here, HD), F32)
                dv = jnp.zeros((here, HD), F32)
                for h in range(group):
                    col = aligned(unit * group + h, HD)
                    q = q_all[:, col]
                    o = o_all[:, col]
                    s = lax.dot_general(kv_all[0, g, low:], q, dims_last, preferred_element_type=F32)
                    dp = lax.dot_general(kv_all[1, g, low:], o, dims_last, preferred_element_type=F32)
                    s = s + bias[:here]
                    top = jnp.max(s, axis=0, keepdims=True)
                    e = jnp.exp2((s - top) * to_log2)
                    inv = 1.0 / jnp.sum(e, axis=0, keepdims=True)
                    delta = jnp.sum(e * dp, axis=0, keepdims=True) * inv
                    prob = e * inv
                    ds = (prob * (dp - delta)).astype(BF16)
                    dv += jnp.dot(prob.astype(BF16), o, preferred_element_type=F32)
                    dk += jnp.dot(ds, q, preferred_element_type=F32)
                    dq = jnp.dot(k_turned[:, :here], ds, preferred_element_type=F32) * scale
                    dq_buf[unit, :, h * HD:(h + 1) * HD] = dq.T.astype(BF16)
                dk_sum[:here] += dk
                dv_sum[:here] += dv
                dq_out(unit, 1 if blocks <= held else None)
                if blocks == 2 and reach > 1 and turn + 1 < kvh:
                    @pl.when((n == per // group // 2 - 1) & goes_on(turn + 1, 1))
                    def _():
                        pass_kv(turn + 1, 1)

                return carry

            with jax.named_scope('attend'):
                lax.fori_loop(0, per // group, one_unit, 0)
            for e in range(blocks):
                at = (blocks - 1 - e) * rows
                for which, sums in enumerate((dk_sum, dv_sum)):
                    col = aligned(core * 2 * kvh + which * kvh + g, HD)
                    for p in range(2):
                        part = sums[at + p * tok:at + (p + 1) * tok]
                        if which == 0:
                            part = part * scale
                        kv_grads[e, p, :, col] = part.astype(BF16)

        if blocks <= held:
            far_out(chips // 2 + 1 if blocks == 1 and early else 2)

    def kvg_copy(e):
        part = kv_grads.at[e, 1 - core, :, aligned(core, span)]
        return remote(part, part, kvg_sent.at[e], kvg_got.at[e], partner)

    for blocks in range(1, reach + 2):
        @pl.when(jnp.minimum(chip, reach) + 1 == blocks)
        def _():
            attend(blocks)
            for e in range(blocks):
                kvg_copy(e).start()

    def kvg_wait(e):
        with jax.named_scope('kvg_wait'):
            part = kv_grads.at[e, core, :, aligned(1 - core, span)]
            pltpu.make_async_copy(part, part, kvg_got.at[e]).wait()

    with jax.named_scope('w_wait'):
        for copy in local:
            copy.wait()
        theirs = weights.at[aligned(1 - core, feats)]
        pltpu.make_async_copy(theirs, theirs, w_got.at[0]).wait()

    def grads_wait(b):
        with jax.named_scope('g_wait'):
            pltpu.make_async_copy(grads.at[b], grads.at[b], g_got.at[b]).wait()

    for b in range(chips):
        @pl.when((chip == b) & (b // (chips // 2) != core))
        def _():
            grads_wait(b)

    def right_copy(d, k):
        here = right_buf.at[d, k]
        return remote(here, here, right_sent.at[0], right_got.at[d - 1, k],
                      (sec, jnp.minimum(me + 2, count - 2 + core)))

    def left_copy(d, k):
        here = left_buf.at[d, k]
        return remote(here, here, left_sent.at[0], left_got.at[d, k],
                      (sec, jnp.maximum(me - 2, core)))

    def final_copy(k):
        return remote(final.at[k], out_ref.at[:, aligned(k, cw)], final_sent.at[0], final_got.at[k],
                      (jnp.maximum(sec - 1, 0), me))

    def product(d, k):
        acc[...] = jnp.dot(grads[d], weights[:, aligned(k, cw)], preferred_element_type=F32)

    def kv_product(e, k):
        acc[...] += jnp.dot(kv_grads[e, core], kv_weights[:, aligned(k, cw)],
                            preferred_element_type=F32)

    def pass_right(d, k):
        with jax.named_scope('r_prod'):
            product(d, k)

        @pl.when(chip > 0)
        def _():
            with jax.named_scope('r_wait'):
                right_copy(d, k).wait_recv()
            acc[...] += right_buf[d, k].astype(F32)

        right_buf[d, k] = acc[...].astype(BF16)
        right_copy(d, k).start()

    def pass_left(d, k):
        with jax.named_scope('l_prod'):
            product(d, k)

            @pl.when(chip - d <= reach)
            def _():
                kv_product(jnp.minimum(chip - d, reach), k)

        @pl.when(chip < last)
        def _():
            with jax.named_scope('l_wait'):
                left_copy(d, k).wait_recv()
            acc[...] += left_buf[d, k].astype(F32)

        left_buf[d, k] = acc[...].astype(BF16)
        left_copy(d, k).start()

    def finish(k):
        with jax.named_scope('f_prod'):
            product(chip, k)
            kv_product(0, k)

        @pl.when(chip > 0)
        def _():
            with jax.named_scope('f_wait_r'):
                right_copy(chip, k).wait_recv()
            acc[...] += right_buf[chip, k].astype(F32)

        @pl.when(chip < last)
        def _():
            with jax.named_scope('f_wait_l'):
                left_copy(chip, k).wait_recv()
            acc[...] += left_buf[chip, k].astype(F32)

        final[k] = acc[...].astype(BF16)

        @pl.when(sec > 0)
        def _():
            final_copy(k).start()

    def each(first, end, act):
        def one(k, carry):
            act(k)
            return carry

        lax.fori_loop(first, end, one, 0)

    lag = 4
    leads_right = chip < chips // 2

    if early:
        @pl.when(chip == 0)
        def _():
            grads_wait(1)
            far_out(2, chips // 2 + 1)
            each(0, early, lambda k: pass_right(1, k))

    for i in range(chips - 1):
        far, near = chips - 1 - i, i
        to_right = chip < far
        to_left = chip > near
        begin = early if i == chips - 2 else 0

        @pl.when(to_right)
        def _():
            if begin == 0:
                grads_wait(far)

        @pl.when(to_left)
        def _():
            grads_wait(near)

        for e in range(1, reach + 1):
            @pl.when(chip == near + e)
            def _():
                kvg_wait(e)

        if i == min(1, chips - 2):
            kvg_wait(0)

        def one(step):
            k_right = step - jnp.where(leads_right, 0, lag)
            k_left = step - jnp.where(leads_right, lag, 0)

            @pl.when(to_right & (k_right >= begin) & (k_right < chunks))
            def _():
                pass_right(far, k_right)

            @pl.when(to_left & (k_left >= 0) & (k_left < chunks))
            def _():
                pass_left(near, k_left)

            if i == 1 and early:
                @pl.when((chip == 1) & (k_left >= 0) & (k_left < early))
                def _():
                    finish(k_left)

        each(0, chunks + lag, one)

    each(0, early, lambda k: pl.when(chip != 1)(lambda: finish(k)))
    each(early, chunks, finish)

    def sent(part, sem):
        pltpu.make_async_copy(part, part, sem).wait()

    with jax.named_scope('drain'):
        for c in range(chips):
            @pl.when(chip == c)
            def _():
                pieces = kvh * ((2 if c < last else 0) + 1) + (2 if direct and c == last - 2 else 0)
                sent(q_all.at[:, :pieces * HD], kv_sent.at[0])
                relays = kvh * min(c, reach - 1) if c < last else 0
                relays -= 1 if direct and c == last - 1 else 0
                if relays:
                    sent(q_all.at[:, :2 * relays * HD], kv_passed.at[0])

        for which in range(2):
            qo_partner(which).wait_send()
        w_copy.wait_send()

        @pl.when(chip // (chips // 2) == core)
        def _():
            sent(dq_buf.at[:units - chip_heads // group // 2], dq_sent.at[0])

        @pl.when(chip // (chips // 2) != core)
        def _():
            sent(dq_buf, dq_sent.at[0])

        for e in range(reach + 1):
            @pl.when(chip >= e)
            def _():
                kvg_copy(e).wait_send()

        for c in range(chips):
            @pl.when(chip == c)
            def _():
                if c < last:
                    sent(right_buf.at[c + 1:], right_sent.at[0])
                if c > 0:
                    sent(left_buf.at[:c], left_sent.at[0])

        @pl.when(sec > 0)
        def _():
            sent(final, final_sent.at[0])

        @pl.when(sec < sections - 1)
        def _():
            each(0, chunks, lambda k: final_copy(k).wait_recv())


def body(queries, keys, values, out_grad, documents, query_weight, key_weight, value_weight):
    sections = lax.axis_size("section")
    count = lax.axis_size("seq")
    tok = queries.shape[1]
    total = tok * count
    kv = keys.shape[2] // HD
    feats = query_weight.shape[1]
    heads = feats // HD
    width = query_weight.shape[2]
    chips = count // 2
    rows = 2 * tok
    reach = -(-(total // 2) // rows)
    group = 2
    cw = min(256, width)
    chunks = width // cw
    units = chips * heads // group
    kvh = kv // 2
    slots = (reach + 1) * rows
    dma = pltpu.SemaphoreType.DMA
    anywhere = pl.BlockSpec(memory_space=pl.ANY)
    vmem = pl.BlockSpec(memory_space=pltpu.VMEM)
    out = pl.pallas_call(
        functools.partial(kernel, (sections, count, tok, heads, kv, width, cw, group, reach)),
        out_shape=pltpu.VMEM((tok, width), BF16),
        in_specs=[anywhere] * 4 + [vmem] + [anywhere] * 3,
        out_specs=vmem,
        scratch_shapes=[
            pltpu.VMEM((rows, chips * feats), BF16),
            pltpu.VMEM((rows, chips * feats), BF16),
            pltpu.VMEM((2, kvh, slots, HD), BF16),
            pltpu.VMEM((HD, slots), BF16),
            pltpu.VMEM((slots, rows), F32),
            pltpu.VMEM((slots, HD), F32),
            pltpu.VMEM((slots, HD), F32),
            pltpu.VMEM((units, rows, group * HD), BF16),
            pltpu.VMEM((chips, tok, 2 * feats), BF16),
            pltpu.VMEM((reach + 1, 2, tok, 2 * kv * HD), BF16),
            pltpu.VMEM((2 * feats, width), BF16),
            pltpu.VMEM((2 * kv * HD, width), BF16),
            pltpu.VMEM((chips, chunks, tok, cw), BF16),
            pltpu.VMEM((chips, chunks, tok, cw), BF16),
            pltpu.VMEM((tok, cw), F32),
            pltpu.VMEM((chunks, tok, cw), BF16),
            dma((2,)),
            dma((2, 2)),
            dma((1,)),
            dma((2, kvh, reach + 1)),
            dma((1,)),
            dma((5,)),
            dma((1,)),
            dma((1,)),
            dma((1,)),
            dma((chips,)),
            dma((reach + 1,)),
            dma((reach + 1,)),
            dma((1,)),
            dma((chips - 1, chunks)),
            dma((1,)),
            dma((chips - 1, chunks)),
            dma((1,)),
            dma((chunks,)),
        ],
        compiler_params=pltpu.CompilerParams(
            collective_id=0, has_side_effects=True, vmem_limit_bytes=60 * 1024 * 1024),
        name="attention_back",
    )(queries[0], keys[0], values[0], out_grad[0], documents,
      query_weight[0], key_weight[0], value_weight[0])
    return out[None]


def solution(mesh):
    in_specs = (
        P("section", "seq", None),
        P("section", "seq", None),
        P("section", "seq", None),
        P("section", "seq", None),
        P("section", None),
        P("section", "seq", None),
        P("section", None, None),
        P("section", None, None),
    )
    out_specs = P("section", "seq", None)
    return jax.shard_map(body, mesh=mesh, in_specs=in_specs, out_specs=out_specs, check_vma=False)
```

```python
import functools
import math

import jax
import jax.numpy as jnp
from jax import lax
from jax.experimental import pallas as pl
from jax.experimental.pallas import tpu as pltpu
from jax.sharding import PartitionSpec as P

HD = 128
MESH = pl.DeviceIdType.MESH
F32 = jnp.float32
BF16 = jnp.bfloat16


def aligned(index, size):
    return pl.ds(pl.multiple_of(index * size, size), size)


def kernel(dims, q_in, k_in, v_in, o_in, ids_ref, wq_in, wk_in, wv_in, out_ref,
           q_all, o_all, kv_own_all, kv_all, k_turned, bias, dk_sum, dv_sum, dq_buf, grads, kv_grads,
           weights, kv_weights, right_buf, left_buf, acc, final,
           stage_got, qo_sent, qo_got, kv_sent, kv_got, kv_passed, w_local, w_sent, w_got,
           dq_sent, g_got, kvg_sent, kvg_got,
           right_sent, right_got, left_sent, left_got, final_sent, final_got):
    sections, count, tok, heads, kv, width, cw, group, reach = dims
    chips = count // 2
    rows = 2 * tok
    feats = heads * HD
    chip_heads = 2 * heads
    own_heads = chips * heads
    units = own_heads // group
    half_feats = own_heads * HD
    kvh = kv // 2
    per = own_heads // kvh
    chunks = width // cw
    span = 2 * kvh * HD
    scale = 1.0 / math.sqrt(HD)
    to_log2 = scale * math.log2(math.e)
    sec = lax.axis_index("section")
    me = lax.axis_index("seq")
    chip = me // 2
    core = me % 2
    partner = (sec, me + 1 - 2 * core)
    last = chips - 1

    def remote(src, dst, send_sem, recv_sem, device):
        return pltpu.make_async_remote_copy(
            src_ref=src, dst_ref=dst, send_sem=send_sem, recv_sem=recv_sem,
            device_id=device, device_id_type=MESH)

    kv_in = (k_in, v_in)
    right = jnp.minimum(chip + 1, last)

    def kv_head(half, g):
        return pl.ds(pl.multiple_of((half * kvh + g) * HD, HD), HD)

    def kv_right(which, g, p):
        return remote(kv_own_all.at[which, :, kv_head(p, g)],
                      kv_all.at[which, g, pl.ds(pl.multiple_of((reach - 1) * rows + core * tok, tok), tok)],
                      kv_sent.at[0], kv_got.at[which, g, 1], (sec, 2 * right + p))

    def kv_direct(which, g, p):
        return remote(kv_own_all.at[which, :, kv_head(p, g)],
                      kv_all.at[which, g, pl.ds(pl.multiple_of((reach - 2) * rows + core * tok, tok), tok)],
                      kv_sent.at[0], kv_got.at[which, g, 2], (sec, 2 * last + p))

    def kv_partner(which, g):
        return remote(kv_own_all.at[which, :, kv_head(1 - core, g)],
                      kv_all.at[which, g, pl.ds(pl.multiple_of(reach * rows + core * tok, tok), tok)],
                      kv_sent.at[0], kv_got.at[which, g, 0], partner)

    def kv_own(which, g):
        return pltpu.make_async_copy(
            kv_in[which].at[:, kv_head(core, g)],
            kv_all.at[which, g, pl.ds(pl.multiple_of(reach * rows + core * tok, tok), tok)],
            kv_got.at[which, g, 0])

    def kv_block(which, g, e):
        return kv_all.at[which, g, pl.ds((reach - e) * rows, rows)]

    def kv_relay(which, g, e):
        return remote(kv_block(which, g, e), kv_block(which, g, e + 1),
                      kv_passed.at[0], kv_got.at[which, g, e + 1],
                      (sec, 2 * right + core))

    def kv_wait(which, g, e):
        part = kv_block(which, g, e)
        pltpu.make_async_copy(part, part, kv_got.at[which, g, e]).wait()

    def pass_kv(g, e):
        with jax.named_scope('relay'):
            for which in range(2):
                kv_wait(which, g, e)
                kv_relay(which, g, e).start()

    def qo_partner(which):
        return remote((q_in, o_in)[which].at[:, aligned(1 - core, half_feats)],
                      (q_all, o_all)[which].at[aligned(core, tok)],
                      qo_sent.at[which], qo_got.at[which, 0], partner)

    def qo_own(which):
        return pltpu.make_async_copy((q_in, o_in)[which].at[:, aligned(core, half_feats)],
                                     (q_all, o_all)[which].at[aligned(core, tok)],
                                     qo_got.at[which, 1])

    w_copy = remote(wq_in, weights.at[aligned(core, feats)], w_sent.at[0], w_got.at[0], partner)

    direct = reach > 1 and chips > 2

    def goes_on(g, e):
        return chip < (last - 1 if direct and g == 0 and e == 1 else last)

    def send_right(g):
        if direct and g == 0:
            @pl.when(chip == last - 2)
            def _():
                for p in range(2):
                    for which in range(2):
                        kv_direct(which, g, p).start()

        @pl.when(chip < last)
        def _():
            for p in range(2):
                for which in range(2):
                    kv_right(which, g, p).start()

    staged = [pltpu.make_async_copy(kv_in[which], kv_own_all.at[which], stage_got.at[which])
              for which in range(2)]
    for copy in staged:
        copy.start()
    for which in range(2):
        qo_own(which).start()
    for g in range(kvh):
        for which in range(2):
            kv_own(which, g).start()
    local = [pltpu.make_async_copy(wq_in, weights.at[aligned(core, feats)], w_local.at[0])]
    for r in range(2):
        part = slice(r * kvh * HD, (r + 1) * kvh * HD)
        for which, source in enumerate((wk_in, wv_in)):
            base = r * span + which * kvh * HD
            local.append(pltpu.make_async_copy(
                source.at[part], kv_weights.at[base:base + kvh * HD],
                w_local.at[1 + 2 * r + which]))
    barrier = pltpu.get_barrier_semaphore()

    def greet(device):
        pl.semaphore_signal(barrier, inc=1, device_id=device, device_id_type=MESH)

    for off in range(1, count):
        greet((sec, lax.rem(me + off, count)))

    @pl.when(sec > 0)
    def _():
        greet((sec - 1, me))

    @pl.when(sec < sections - 1)
    def _():
        greet((sec + 1, me))

    above = jnp.where(sec > 0, 1, 0)
    below = jnp.where(sec < sections - 1, 1, 0)
    with jax.named_scope('barrier'):
        pl.semaphore_wait(barrier, count - 1 + above + below)

    for copy in staged:
        copy.wait()

    send_right(0)
    for g in range(1, kvh):
        send_right(g)

    for g in range(kvh):
        for which in range(2):
            kv_partner(which, g).start()
    for which in range(2):
        qo_partner(which).start()

    w_copy.start()
    for copy in local:
        copy.start()

    @pl.when(sec == sections - 1)
    def _():
        out_ref[...] = jnp.zeros_like(out_ref)

    q_ids = ids_ref[:, aligned(chip, rows)]

    def set_bias(blocks):
        here = blocks * rows
        first = pl.ds(pl.multiple_of((chip + 1 - blocks) * rows, rows), here)
        k_ids = jnp.broadcast_to(ids_ref[:, first], (HD, here)).T[:, :1]
        same = k_ids == q_ids
        j = lax.broadcasted_iota(jnp.int32, (here, rows), 0)
        i = lax.broadcasted_iota(jnp.int32, (here, rows), 1) + (blocks - 1) * rows
        bias[:here] = jnp.where(same & (j <= i), 0.0, -jnp.inf)

    for blocks in range(1, reach + 2):
        @pl.when(jnp.minimum(chip, reach) + 1 == blocks)
        def _():
            with jax.named_scope('bias'):
                set_bias(blocks)

    for g in range(kvh):
        for e in range(1, reach):
            from_chip = e if g == 0 else max(e, 2)

            @pl.when((chip >= from_chip) & goes_on(g, e))
            def _():
                pass_kv(g, e)

    with jax.named_scope('qo_wait'):
        for which in range(2):
            buf = (q_all, o_all)[which]
            qo_own(which).wait()
            part = buf.at[aligned(1 - core, tok)]
            pltpu.make_async_copy(part, part, qo_got.at[which, 0]).wait()

    def dq_place(unit):
        head = unit * group
        target = core * (chips // 2) + head // chip_heads
        piece = (head % chip_heads) // group
        return target, piece

    def dq_copy(unit, p):
        target, piece = dq_place(unit)
        return remote(dq_buf.at[unit, p * tok:(p + 1) * tok],
                      grads.at[chip, :, aligned(piece, group * HD)],
                      dq_sent.at[0], g_got.at[chip], (sec, 2 * target + p))

    def dq_out(unit, reaches=None):
        target, piece = dq_place(unit)
        for p in range(2):
            @pl.when((2 * target + p != me) if reaches is None else (2 * target + p != me) & (target <= reaches))
            def _():
                dq_copy(unit, p).start()

            @pl.when(2 * target + p == me)
            def _():
                grads[chip, :, aligned(piece, group * HD)] = dq_buf[unit, p * tok:(p + 1) * tok]

    dims_last = (((1,), (1,)), ((), ()))

    early = chunks * 3 // 8 if chips > 3 else 0
    early_left = chunks // 4 if chips > 3 else 0

    def far_out(first, end=chips):
        def far_unit(n, carry):
            unit = units - 1 - n
            target, _ = dq_place(unit)

            @pl.when((target >= first) & (target < end))
            def _():
                for p in range(2):
                    dq_copy(unit, p).start()

            return carry

        lax.fori_loop(0, units, far_unit, 0)

    held = min(2, reach)
    batch = 1

    def attend(blocks):
        here = blocks * rows
        low = (reach + 1 - blocks) * rows
        for turn in range(kvh):
            g = jnp.where(core == 0, kvh - 1 - turn, turn) if blocks == 1 else turn
            with jax.named_scope('kv_wait'):
                for e in range(blocks):
                    if 1 <= e < reach:
                        @pl.when(~goes_on(g, e))
                        def _():
                            kv_wait(0, g, e)
                            kv_wait(1, g, e)
                    else:
                        kv_wait(0, g, e)
                        kv_wait(1, g, e)
            k_turned[:, :here] = kv_all[0, g, low:].T
            dk_sum[:here] = jnp.zeros((here, HD), F32)
            dv_sum[:here] = jnp.zeros((here, HD), F32)

            def unit_of(n, h):
                return g * (per // group) + n * batch + h // group

            def one_batch(n, carry):
                dk = jnp.zeros((here, HD), F32)
                dv = jnp.zeros((here, HD), F32)
                heads_here = range(batch * group)
                cols = [aligned(unit_of(n, h) * group + h % group, HD) for h in heads_here]
                scores, dprobs = {}, {}

                def start_head(h):
                    scores[h] = lax.dot_general(kv_all[0, g, low:], q_all[:, cols[h]], dims_last,
                                                preferred_element_type=F32) + bias[:here]
                    dprobs[h] = lax.dot_general(kv_all[1, g, low:], o_all[:, cols[h]], dims_last,
                                                preferred_element_type=F32)

                def weigh(h):
                    s, dp = scores.pop(h), dprobs.pop(h)
                    top = jnp.max(s, axis=0, keepdims=True)
                    e = jnp.exp2((s - top) * to_log2)
                    inv = 1.0 / jnp.sum(e, axis=0, keepdims=True)
                    delta = jnp.sum(e * dp, axis=0, keepdims=True) * inv
                    prob = e * inv
                    return prob.astype(BF16), (prob * (dp - delta)).astype(BF16)

                start_head(0)
                for h in heads_here:
                    if h + 1 < len(heads_here):
                        start_head(h + 1)
                    prob, ds = weigh(h)
                    dv += jnp.dot(prob, o_all[:, cols[h]], preferred_element_type=F32)
                    dk += jnp.dot(ds, q_all[:, cols[h]], preferred_element_type=F32)
                    dq = jnp.dot(k_turned[:, :here], ds, preferred_element_type=F32) * scale
                    at = h % group
                    dq_buf[unit_of(n, h), :, at * HD:(at + 1) * HD] = dq.T.astype(BF16)
                if at == group - 1:
                        dq_out(unit_of(n, h), 1 if blocks <= held else None)
                dk_sum[:here] += dk
                dv_sum[:here] += dv
                if blocks == 2 and reach > 1 and turn + 1 < kvh:
                    @pl.when((n == per // group // batch // 2 - 1) & goes_on(turn + 1, 1))
                    def _():
                        pass_kv(turn + 1, 1)

                return carry

            with jax.named_scope('attend'):
                lax.fori_loop(0, per // group // batch, one_batch, 0)
            for e in range(blocks):
                at = (blocks - 1 - e) * rows
                for which, sums in enumerate((dk_sum, dv_sum)):
                    col = aligned(core * 2 * kvh + which * kvh + g, HD)
                    for p in range(2):
                        part = sums[at + p * tok:at + (p + 1) * tok]
                        if which == 0:
                            part = part * scale
                        kv_grads[e, p, :, col] = part.astype(BF16)

        if blocks <= held:
            far_out(chips // 2 + 1 if blocks == 1 and early else 2)

    def kvg_copy(e):
        part = kv_grads.at[e, 1 - core, :, aligned(core, span)]
        return remote(part, part, kvg_sent.at[e], kvg_got.at[e], partner)

    for blocks in range(1, reach + 2):
        @pl.when(jnp.minimum(chip, reach) + 1 == blocks)
        def _():
            attend(blocks)
            for e in range(blocks):
                kvg_copy(e).start()

    def kvg_wait(e):
        with jax.named_scope('kvg_wait'):
            part = kv_grads.at[e, core, :, aligned(1 - core, span)]
            pltpu.make_async_copy(part, part, kvg_got.at[e]).wait()

    with jax.named_scope('w_wait'):
        for copy in local:
            copy.wait()
        theirs = weights.at[aligned(1 - core, feats)]
        pltpu.make_async_copy(theirs, theirs, w_got.at[0]).wait()

    def grads_wait(b):
        with jax.named_scope('g_wait'):
            pltpu.make_async_copy(grads.at[b], grads.at[b], g_got.at[b]).wait()

    def right_copy(d, k):
        here = right_buf.at[d, k]
        return remote(here, here, right_sent.at[0], right_got.at[d - 1, k],
                      (sec, jnp.minimum(me + 2, count - 2 + core)))

    def left_copy(d, k):
        here = left_buf.at[d, k]
        return remote(here, here, left_sent.at[0], left_got.at[d, k],
                      (sec, jnp.maximum(me - 2, core)))

    def final_copy(k):
        return remote(final.at[k], out_ref.at[:, aligned(k, cw)], final_sent.at[0], final_got.at[k],
                      (jnp.maximum(sec - 1, 0), me))

    def product(d, k):
        acc[...] = jnp.dot(grads[d], weights[:, aligned(k, cw)], preferred_element_type=F32)

    def kv_product(e, k):
        acc[...] += jnp.dot(kv_grads[e, core], kv_weights[:, aligned(k, cw)],
                            preferred_element_type=F32)

    def pass_right(d, k):
        with jax.named_scope('r_prod'):
            product(d, k)

        @pl.when(chip > 0)
        def _():
            with jax.named_scope('r_wait'):
                right_copy(d, k).wait_recv()
            acc[...] += right_buf[d, k].astype(F32)

        right_buf[d, k] = acc[...].astype(BF16)
        right_copy(d, k).start()

    def pass_left(d, k):
        with jax.named_scope('l_prod'):
            product(d, k)

            @pl.when(chip - d <= reach)
            def _():
                kv_product(jnp.minimum(chip - d, reach), k)

        @pl.when(chip < last)
        def _():
            with jax.named_scope('l_wait'):
                left_copy(d, k).wait_recv()
            acc[...] += left_buf[d, k].astype(F32)

        left_buf[d, k] = acc[...].astype(BF16)
        left_copy(d, k).start()

    def finish(k):
        with jax.named_scope('f_prod'):
            product(chip, k)
            kv_product(0, k)

        @pl.when(chip > 0)
        def _():
            with jax.named_scope('f_wait_r'):
                right_copy(chip, k).wait_recv()
            acc[...] += right_buf[chip, k].astype(F32)

        @pl.when(chip < last)
        def _():
            with jax.named_scope('f_wait_l'):
                left_copy(chip, k).wait_recv()
            acc[...] += left_buf[chip, k].astype(F32)

        final[k] = acc[...].astype(BF16)

        @pl.when(sec > 0)
        def _():
            final_copy(k).start()

    def each(first, end, act):
        def one(k, carry):
            act(k)
            return carry

        lax.fori_loop(first, end, one, 0)

    lag = 4
    leads_right = chip < chips // 2

    if early:
        @pl.when(chip == 0)
        def _():
            grads_wait(1)
            far_out(2, chips // 2 + 1)
            each(0, early, lambda k: pass_right(1, k))

    for i in range(chips - 1):
        far, near = chips - 1 - i, i
        to_right = chip < far
        to_left = chip > near
        begin = early if i == chips - 2 else 0
        begin_left = early_left if i == chips - 2 else 0

        if early_left and i == chips - 3:
            @pl.when(chip == last)
            def _():
                grads_wait(chips - 2)
                kvg_wait(1)
                each(0, early_left, lambda k: pass_left(chips - 2, k))

        @pl.when(to_right)
        def _():
            if begin == 0:
                grads_wait(far)

        if begin_left == 0:
            @pl.when(to_left)
            def _():
                grads_wait(near)

            for e in range(1, reach + 1):
                @pl.when(chip == near + e)
                def _():
                    kvg_wait(e)

        if i == min(1, chips - 2):
            kvg_wait(0)
            for b in range(chips):
                @pl.when((chip == b) & (b // (chips // 2) != core))
                def _():
                    grads_wait(b)

        def one(step):
            k_right = step - jnp.where(leads_right, 0, lag)
            k_left = step - jnp.where(leads_right, lag, 0)

            @pl.when(to_right & (k_right >= begin) & (k_right < chunks))
            def _():
                pass_right(far, k_right)

            @pl.when(to_left & (k_left >= begin_left) & (k_left < chunks))
            def _():
                pass_left(near, k_left)

            if i == 1 and early:
                @pl.when((chip == 1) & (k_left >= 0) & (k_left < early))
                def _():
                    finish(k_left)

            if early_left and i == chips - 3:
                @pl.when((chip == chips - 2) & (k_right >= 0) & (k_right < early_left))
                def _():
                    finish(k_right)

        each(0, chunks + lag, one)

    done = jnp.where(chip == chips - 2, early_left, 0)
    each(jnp.where(chip == 1, early, done), chunks, finish)

    def sent(part, sem):
        pltpu.make_async_copy(part, part, sem).wait()

    with jax.named_scope('drain'):
        for c in range(chips):
            @pl.when(chip == c)
            def _():
                pieces = kvh * ((2 if c < last else 0) + 1) + (2 if direct and c == last - 2 else 0)
                sent(q_all.at[:, :pieces * HD], kv_sent.at[0])
                relays = kvh * min(c, reach - 1) if c < last else 0
                relays -= 1 if direct and c == last - 1 else 0
                if relays:
                    sent(q_all.at[:, :2 * relays * HD], kv_passed.at[0])

        for which in range(2):
            qo_partner(which).wait_send()
        w_copy.wait_send()

        @pl.when(chip // (chips // 2) == core)
        def _():
            sent(dq_buf.at[:units - chip_heads // group // 2], dq_sent.at[0])

        @pl.when(chip // (chips // 2) != core)
        def _():
            sent(dq_buf, dq_sent.at[0])

        for e in range(reach + 1):
            @pl.when(chip >= e)
            def _():
                kvg_copy(e).wait_send()

        for c in range(chips):
            @pl.when(chip == c)
            def _():
                if c < last:
                    sent(right_buf.at[c + 1:], right_sent.at[0])
                if c > 0:
                    sent(left_buf.at[:c], left_sent.at[0])

        @pl.when(sec > 0)
        def _():
            sent(final, final_sent.at[0])

        @pl.when(sec < sections - 1)
        def _():
            each(0, chunks, lambda k: final_copy(k).wait_recv())


def body(queries, keys, values, out_grad, documents, query_weight, key_weight, value_weight):
    sections = lax.axis_size("section")
    count = lax.axis_size("seq")
    tok = queries.shape[1]
    total = tok * count
    kv = keys.shape[2] // HD
    feats = query_weight.shape[1]
    heads = feats // HD
    width = query_weight.shape[2]
    chips = count // 2
    rows = 2 * tok
    reach = -(-(total // 2) // rows)
    group = 2
    cw = min(256, width)
    chunks = width // cw
    units = chips * heads // group
    kvh = kv // 2
    slots = (reach + 1) * rows
    dma = pltpu.SemaphoreType.DMA
    anywhere = pl.BlockSpec(memory_space=pl.ANY)
    vmem = pl.BlockSpec(memory_space=pltpu.VMEM)
    out = pl.pallas_call(
        functools.partial(kernel, (sections, count, tok, heads, kv, width, cw, group, reach)),
        out_shape=pltpu.VMEM((tok, width), BF16),
        in_specs=[anywhere] * 4 + [vmem] + [anywhere] * 3,
        out_specs=vmem,
        scratch_shapes=[
            pltpu.VMEM((rows, chips * feats), BF16),
            pltpu.VMEM((rows, chips * feats), BF16),
            pltpu.VMEM((2, tok, kv * HD), BF16),
            pltpu.VMEM((2, kvh, slots, HD), BF16),
            pltpu.VMEM((HD, slots), BF16),
            pltpu.VMEM((slots, rows), F32),
            pltpu.VMEM((slots, HD), F32),
            pltpu.VMEM((slots, HD), F32),
            pltpu.VMEM((units, rows, group * HD), BF16),
            pltpu.VMEM((chips, tok, 2 * feats), BF16),
            pltpu.VMEM((reach + 1, 2, tok, 2 * kv * HD), BF16),
            pltpu.VMEM((2 * feats, width), BF16),
            pltpu.VMEM((2 * kv * HD, width), BF16),
            pltpu.VMEM((chips, chunks, tok, cw), BF16),
            pltpu.VMEM((chips, chunks, tok, cw), BF16),
            pltpu.VMEM((tok, cw), F32),
            pltpu.VMEM((chunks, tok, cw), BF16),
            dma((2,)),
            dma((2,)),
            dma((2, 2)),
            dma((1,)),
            dma((2, kvh, reach + 1)),
            dma((1,)),
            dma((5,)),
            dma((1,)),
            dma((1,)),
            dma((1,)),
            dma((chips,)),
            dma((reach + 1,)),
            dma((reach + 1,)),
            dma((1,)),
            dma((chips - 1, chunks)),
            dma((1,)),
            dma((chips - 1, chunks)),
            dma((1,)),
            dma((chunks,)),
        ],
        compiler_params=pltpu.CompilerParams(
            collective_id=0, has_side_effects=True, vmem_limit_bytes=60 * 1024 * 1024),
        name="attention_back",
    )(queries[0], keys[0], values[0], out_grad[0], documents,
      query_weight[0], key_weight[0], value_weight[0])
    return out[None]


def solution(mesh):
    in_specs = (
        P("section", "seq", None),
        P("section", "seq", None),
        P("section", "seq", None),
        P("section", "seq", None),
        P("section", None),
        P("section", "seq", None),
        P("section", None, None),
        P("section", None, None),
    )
    out_specs = P("section", "seq", None)
    return jax.shard_map(body, mesh=mesh, in_specs=in_specs, out_specs=out_specs, check_vma=False)
```

```python
import functools
import math

import jax
import jax.numpy as jnp
from jax import lax
from jax.experimental import pallas as pl
from jax.experimental.pallas import tpu as pltpu
from jax.sharding import PartitionSpec as P

HD = 128
MESH = pl.DeviceIdType.MESH
F32 = jnp.float32
BF16 = jnp.bfloat16


def aligned(index, size):
    return pl.ds(pl.multiple_of(index * size, size), size)


def kernel(dims, q_in, k_in, v_in, o_in, ids_in, wq_in, wk_in, wv_in, out_ref,
           ids_ref, q_all, o_all, kv_own_all, kv_all, k_turned, bias, dk_sum, dv_sum, dq_buf, grads, kv_grads,
           weights, kv_weights, right_buf, left_buf, acc, final,
           ids_got, stage_got, qo_sent, qo_got, kv_sent, kv_got, kv_passed, w_local, w_sent, w_got,
           dq_sent, g_got, kvg_sent, kvg_got,
           right_sent, right_got, left_sent, left_got, final_sent, final_got):
    sections, count, tok, heads, kv, width, cw, group, reach = dims
    chips = count // 2
    rows = 2 * tok
    feats = heads * HD
    chip_heads = 2 * heads
    own_heads = chips * heads
    units = own_heads // group
    half_feats = own_heads * HD
    kvh = kv // 2
    per = own_heads // kvh
    chunks = width // cw
    span = 2 * kvh * HD
    scale = 1.0 / math.sqrt(HD)
    to_log2 = scale * math.log2(math.e)
    sec = lax.axis_index("section")
    me = lax.axis_index("seq")
    chip = me // 2
    core = me % 2
    partner = (sec, me + 1 - 2 * core)
    last = chips - 1

    def remote(src, dst, send_sem, recv_sem, device):
        return pltpu.make_async_remote_copy(
            src_ref=src, dst_ref=dst, send_sem=send_sem, recv_sem=recv_sem,
            device_id=device, device_id_type=MESH)

    kv_in = (k_in, v_in)
    right = jnp.minimum(chip + 1, last)

    def kv_head(half, g):
        return pl.ds(pl.multiple_of((half * kvh + g) * HD, HD), HD)

    def kv_right(which, g, p):
        return remote(kv_own_all.at[which, :, kv_head(p, g)],
                      kv_all.at[which, g, pl.ds(pl.multiple_of((reach - 1) * rows + core * tok, tok), tok)],
                      kv_sent.at[0], kv_got.at[which, g, 1], (sec, 2 * right + p))

    def kv_direct(which, g, p):
        return remote(kv_own_all.at[which, :, kv_head(p, g)],
                      kv_all.at[which, g, pl.ds(pl.multiple_of((reach - 2) * rows + core * tok, tok), tok)],
                      kv_sent.at[0], kv_got.at[which, g, 2], (sec, 2 * last + p))

    def kv_partner(which, g):
        return remote(kv_own_all.at[which, :, kv_head(1 - core, g)],
                      kv_all.at[which, g, pl.ds(pl.multiple_of(reach * rows + core * tok, tok), tok)],
                      kv_sent.at[0], kv_got.at[which, g, 0], partner)

    def kv_own(which, g):
        return pltpu.make_async_copy(
            kv_in[which].at[:, kv_head(core, g)],
            kv_all.at[which, g, pl.ds(pl.multiple_of(reach * rows + core * tok, tok), tok)],
            kv_got.at[which, g, 0])

    def kv_block(which, g, e):
        return kv_all.at[which, g, pl.ds((reach - e) * rows, rows)]

    def kv_relay(which, g, e):
        return remote(kv_block(which, g, e), kv_block(which, g, e + 1),
                      kv_passed.at[0], kv_got.at[which, g, e + 1],
                      (sec, 2 * right + core))

    def kv_wait(which, g, e):
        part = kv_block(which, g, e)
        pltpu.make_async_copy(part, part, kv_got.at[which, g, e]).wait()

    def pass_kv(g, e):
        with jax.named_scope('relay'):
            for which in range(2):
                kv_wait(which, g, e)
                kv_relay(which, g, e).start()

    def qo_partner(which):
        return remote((q_in, o_in)[which].at[:, aligned(1 - core, half_feats)],
                      (q_all, o_all)[which].at[aligned(core, tok)],
                      qo_sent.at[which], qo_got.at[which, 0], partner)

    def qo_own(which):
        return pltpu.make_async_copy((q_in, o_in)[which].at[:, aligned(core, half_feats)],
                                     (q_all, o_all)[which].at[aligned(core, tok)],
                                     qo_got.at[which, 1])

    w_copy = remote(wq_in, weights.at[aligned(core, feats)], w_sent.at[0], w_got.at[0], partner)

    direct = reach > 1 and chips > 2

    def goes_on(g, e):
        return chip < (last - 1 if direct and g == 0 and e == 1 else last)

    def send_right(g):
        if direct and g == 0:
            @pl.when(chip == last - 2)
            def _():
                for p in range(2):
                    for which in range(2):
                        kv_direct(which, g, p).start()

        @pl.when(chip < last)
        def _():
            for p in range(2):
                for which in range(2):
                    kv_right(which, g, p).start()

    staged = [pltpu.make_async_copy(kv_in[which], kv_own_all.at[which], stage_got.at[which])
              for which in range(2)]
    ids_copy = pltpu.make_async_copy(ids_in, ids_ref, ids_got.at[0])
    for copy in staged + [ids_copy]:
        copy.start()
    for which in range(2):
        qo_own(which).start()
    for g in range(kvh):
        for which in range(2):
            kv_own(which, g).start()
    local = [pltpu.make_async_copy(wq_in, weights.at[aligned(core, feats)], w_local.at[0])]
    for r in range(2):
        part = slice(r * kvh * HD, (r + 1) * kvh * HD)
        for which, source in enumerate((wk_in, wv_in)):
            base = r * span + which * kvh * HD
            local.append(pltpu.make_async_copy(
                source.at[part], kv_weights.at[base:base + kvh * HD],
                w_local.at[1 + 2 * r + which]))
    barrier = pltpu.get_barrier_semaphore()

    def greet(device):
        pl.semaphore_signal(barrier, inc=1, device_id=device, device_id_type=MESH)

    for off in range(1, count):
        greet((sec, lax.rem(me + off, count)))

    @pl.when(sec > 0)
    def _():
        greet((sec - 1, me))

    @pl.when(sec < sections - 1)
    def _():
        greet((sec + 1, me))

    above = jnp.where(sec > 0, 1, 0)
    below = jnp.where(sec < sections - 1, 1, 0)
    with jax.named_scope('barrier'):
        pl.semaphore_wait(barrier, count - 1 + above + below)

    for copy in staged:
        copy.wait()

    send_right(0)
    for g in range(1, kvh):
        send_right(g)

    for g in range(kvh):
        for which in range(2):
            kv_partner(which, g).start()
    for which in range(2):
        qo_partner(which).start()

    w_copy.start()
    for copy in local:
        copy.start()

    @pl.when(sec == sections - 1)
    def _():
        out_ref[...] = jnp.zeros_like(out_ref)

    ids_copy.wait()
    q_ids = ids_ref[:, aligned(chip, rows)]

    def set_bias(blocks):
        here = blocks * rows
        first = pl.ds(pl.multiple_of((chip + 1 - blocks) * rows, rows), here)
        k_ids = jnp.broadcast_to(ids_ref[:, first], (HD, here)).T[:, :1]
        same = k_ids == q_ids
        j = lax.broadcasted_iota(jnp.int32, (here, rows), 0)
        i = lax.broadcasted_iota(jnp.int32, (here, rows), 1) + (blocks - 1) * rows
        bias[:here] = jnp.where(same & (j <= i), 0.0, -jnp.inf)

    for blocks in range(1, reach + 2):
        @pl.when(jnp.minimum(chip, reach) + 1 == blocks)
        def _():
            with jax.named_scope('bias'):
                set_bias(blocks)

    for g in range(kvh):
        for e in range(1, reach):
            from_chip = e if g == 0 else max(e, 2)

            @pl.when((chip >= from_chip) & goes_on(g, e))
            def _():
                pass_kv(g, e)

    with jax.named_scope('qo_wait'):
        for which in range(2):
            buf = (q_all, o_all)[which]
            qo_own(which).wait()
            part = buf.at[aligned(1 - core, tok)]
            pltpu.make_async_copy(part, part, qo_got.at[which, 0]).wait()

    def dq_place(unit):
        head = unit * group
        target = core * (chips // 2) + head // chip_heads
        piece = (head % chip_heads) // group
        return target, piece

    def dq_copy(unit, p):
        target, piece = dq_place(unit)
        return remote(dq_buf.at[unit, p * tok:(p + 1) * tok],
                      grads.at[chip, :, aligned(piece, group * HD)],
                      dq_sent.at[0], g_got.at[chip], (sec, 2 * target + p))

    def dq_out(unit, reaches=None):
        target, piece = dq_place(unit)
        for p in range(2):
            @pl.when((2 * target + p != me) if reaches is None else (2 * target + p != me) & (target <= reaches))
            def _():
                dq_copy(unit, p).start()

            @pl.when(2 * target + p == me)
            def _():
                grads[chip, :, aligned(piece, group * HD)] = dq_buf[unit, p * tok:(p + 1) * tok]

    dims_last = (((1,), (1,)), ((), ()))

    early = chunks * 3 // 8 if chips > 3 else 0
    early_left = chunks // 4 if chips > 3 else 0

    def far_out(first, end=chips):
        def far_unit(n, carry):
            unit = units - 1 - n
            target, _ = dq_place(unit)

            @pl.when((target >= first) & (target < end))
            def _():
                for p in range(2):
                    dq_copy(unit, p).start()

            return carry

        lax.fori_loop(0, units, far_unit, 0)

    held = min(2, reach)
    batch = 1

    def attend(blocks):
        here = blocks * rows
        low = (reach + 1 - blocks) * rows
        for turn in range(kvh):
            g = jnp.where(core == 0, kvh - 1 - turn, turn) if blocks == 1 else turn
            with jax.named_scope('kv_wait'):
                for e in range(blocks):
                    if 1 <= e < reach:
                        @pl.when(~goes_on(g, e))
                        def _():
                            kv_wait(0, g, e)
                            kv_wait(1, g, e)
                    else:
                        kv_wait(0, g, e)
                        kv_wait(1, g, e)
            k_turned[:, :here] = kv_all[0, g, low:].T
            dk_sum[:here] = jnp.zeros((here, HD), F32)
            dv_sum[:here] = jnp.zeros((here, HD), F32)

            def unit_of(n, h):
                return g * (per // group) + n * batch + h // group

            def one_batch(n, carry):
                dk = jnp.zeros((here, HD), F32)
                dv = jnp.zeros((here, HD), F32)
                heads_here = range(batch * group)
                cols = [aligned(unit_of(n, h) * group + h % group, HD) for h in heads_here]
                scores, dprobs = {}, {}

                def start_head(h):
                    scores[h] = lax.dot_general(kv_all[0, g, low:], q_all[:, cols[h]], dims_last,
                                                preferred_element_type=F32) + bias[:here]
                    dprobs[h] = lax.dot_general(kv_all[1, g, low:], o_all[:, cols[h]], dims_last,
                                                preferred_element_type=F32)

                def weigh(h):
                    s, dp = scores.pop(h), dprobs.pop(h)
                    top = jnp.max(s, axis=0, keepdims=True)
                    e = jnp.exp2((s - top) * to_log2)
                    inv = 1.0 / jnp.sum(e, axis=0, keepdims=True)
                    delta = jnp.sum(e * dp, axis=0, keepdims=True) * inv
                    prob = e * inv
                    return prob.astype(BF16), (prob * (dp - delta)).astype(BF16)

                start_head(0)
                for h in heads_here:
                    if h + 1 < len(heads_here):
                        start_head(h + 1)
                    prob, ds = weigh(h)
                    dv += jnp.dot(prob, o_all[:, cols[h]], preferred_element_type=F32)
                    dk += jnp.dot(ds, q_all[:, cols[h]], preferred_element_type=F32)
                    dq = jnp.dot(k_turned[:, :here], ds, preferred_element_type=F32) * scale
                    at = h % group
                    dq_buf[unit_of(n, h), :, at * HD:(at + 1) * HD] = dq.T.astype(BF16)
                if at == group - 1:
                        dq_out(unit_of(n, h), 1 if blocks <= held else None)
                dk_sum[:here] += dk
                dv_sum[:here] += dv
                if blocks == 2 and reach > 1 and turn + 1 < kvh:
                    @pl.when((n == per // group // batch // 2 - 1) & goes_on(turn + 1, 1))
                    def _():
                        pass_kv(turn + 1, 1)

                return carry

            with jax.named_scope('attend'):
                lax.fori_loop(0, per // group // batch, one_batch, 0)
            for e in range(blocks):
                at = (blocks - 1 - e) * rows
                for which, sums in enumerate((dk_sum, dv_sum)):
                    col = aligned(core * 2 * kvh + which * kvh + g, HD)
                    for p in range(2):
                        part = sums[at + p * tok:at + (p + 1) * tok]
                        if which == 0:
                            part = part * scale
                        kv_grads[e, p, :, col] = part.astype(BF16)

        if blocks <= held:
            far_out(chips // 2 + 1 if blocks == 1 and early else 2)

    def kvg_copy(e):
        part = kv_grads.at[e, 1 - core, :, aligned(core, span)]
        return remote(part, part, kvg_sent.at[e], kvg_got.at[e], partner)

    for blocks in range(1, reach + 2):
        @pl.when(jnp.minimum(chip, reach) + 1 == blocks)
        def _():
            attend(blocks)
            for e in range(blocks):
                kvg_copy(e).start()

    def kvg_wait(e):
        with jax.named_scope('kvg_wait'):
            part = kv_grads.at[e, core, :, aligned(1 - core, span)]
            pltpu.make_async_copy(part, part, kvg_got.at[e]).wait()

    with jax.named_scope('w_wait'):
        for copy in local:
            copy.wait()
        theirs = weights.at[aligned(1 - core, feats)]
        pltpu.make_async_copy(theirs, theirs, w_got.at[0]).wait()

    def grads_wait(b):
        with jax.named_scope('g_wait'):
            pltpu.make_async_copy(grads.at[b], grads.at[b], g_got.at[b]).wait()

    def right_copy(d, k):
        here = right_buf.at[d, k]
        return remote(here, here, right_sent.at[0], right_got.at[d - 1, k],
                      (sec, jnp.minimum(me + 2, count - 2 + core)))

    def left_copy(d, k):
        here = left_buf.at[d, k]
        return remote(here, here, left_sent.at[0], left_got.at[d, k],
                      (sec, jnp.maximum(me - 2, core)))

    def final_copy(k):
        return remote(final.at[k], out_ref.at[:, aligned(k, cw)], final_sent.at[0], final_got.at[k],
                      (jnp.maximum(sec - 1, 0), me))

    def product(d, k):
        acc[...] = jnp.dot(grads[d], weights[:, aligned(k, cw)], preferred_element_type=F32)

    def kv_product(e, k):
        acc[...] += jnp.dot(kv_grads[e, core], kv_weights[:, aligned(k, cw)],
                            preferred_element_type=F32)

    def pass_right(d, k):
        with jax.named_scope('r_prod'):
            product(d, k)

        @pl.when(chip > 0)
        def _():
            with jax.named_scope('r_wait'):
                right_copy(d, k).wait_recv()
            acc[...] += right_buf[d, k].astype(F32)

        right_buf[d, k] = acc[...].astype(BF16)
        right_copy(d, k).start()

    def pass_left(d, k):
        with jax.named_scope('l_prod'):
            product(d, k)

            @pl.when(chip - d <= reach)
            def _():
                kv_product(jnp.minimum(chip - d, reach), k)

        @pl.when(chip < last)
        def _():
            with jax.named_scope('l_wait'):
                left_copy(d, k).wait_recv()
            acc[...] += left_buf[d, k].astype(F32)

        left_buf[d, k] = acc[...].astype(BF16)
        left_copy(d, k).start()

    def finish(k):
        with jax.named_scope('f_prod'):
            product(chip, k)
            kv_product(0, k)

        @pl.when(chip > 0)
        def _():
            with jax.named_scope('f_wait_r'):
                right_copy(chip, k).wait_recv()
            acc[...] += right_buf[chip, k].astype(F32)

        @pl.when(chip < last)
        def _():
            with jax.named_scope('f_wait_l'):
                left_copy(chip, k).wait_recv()
            acc[...] += left_buf[chip, k].astype(F32)

        final[k] = acc[...].astype(BF16)

        @pl.when(sec > 0)
        def _():
            final_copy(k).start()

    def each(first, end, act):
        def one(k, carry):
            act(k)
            return carry

        lax.fori_loop(first, end, one, 0)

    lag = 4
    leads_right = chip < chips // 2

    if early:
        @pl.when(chip == 0)
        def _():
            grads_wait(1)
            far_out(2, chips // 2 + 1)
            each(0, early, lambda k: pass_right(1, k))

    for i in range(chips - 1):
        far, near = chips - 1 - i, i
        to_right = chip < far
        to_left = chip > near
        begin = early if i == chips - 2 else 0
        begin_left = early_left if i == chips - 2 else 0

        if early_left and i == chips - 3:
            @pl.when(chip == last)
            def _():
                grads_wait(chips - 2)
                kvg_wait(1)
                each(0, early_left, lambda k: pass_left(chips - 2, k))

        @pl.when(to_right)
        def _():
            if begin == 0:
                grads_wait(far)

        if begin_left == 0:
            @pl.when(to_left)
            def _():
                grads_wait(near)

            for e in range(1, reach + 1):
                @pl.when(chip == near + e)
                def _():
                    kvg_wait(e)

        if i == min(1, chips - 2):
            kvg_wait(0)
            for b in range(chips):
                @pl.when((chip == b) & (b // (chips // 2) != core))
                def _():
                    grads_wait(b)

        def one(step):
            k_right = step - jnp.where(leads_right, 0, lag)
            k_left = step - jnp.where(leads_right, lag, 0)

            @pl.when(to_right & (k_right >= begin) & (k_right < chunks))
            def _():
                pass_right(far, k_right)

            @pl.when(to_left & (k_left >= begin_left) & (k_left < chunks))
            def _():
                pass_left(near, k_left)

            if i == 1 and early:
                @pl.when((chip == 1) & (k_left >= 0) & (k_left < early))
                def _():
                    finish(k_left)

            if early_left and i == chips - 3:
                @pl.when((chip == chips - 2) & (k_right >= 0) & (k_right < early_left))
                def _():
                    finish(k_right)

        each(0, chunks + lag, one)

    done = jnp.where(chip == chips - 2, early_left, 0)
    each(jnp.where(chip == 1, early, done), chunks, finish)

    def sent(part, sem):
        pltpu.make_async_copy(part, part, sem).wait()

    with jax.named_scope('drain'):
        for c in range(chips):
            @pl.when(chip == c)
            def _():
                pieces = kvh * ((2 if c < last else 0) + 1) + (2 if direct and c == last - 2 else 0)
                sent(q_all.at[:, :pieces * HD], kv_sent.at[0])
                relays = kvh * min(c, reach - 1) if c < last else 0
                relays -= 1 if direct and c == last - 1 else 0
                if relays:
                    sent(q_all.at[:, :2 * relays * HD], kv_passed.at[0])

        for which in range(2):
            qo_partner(which).wait_send()
        w_copy.wait_send()

        @pl.when(chip // (chips // 2) == core)
        def _():
            sent(dq_buf.at[:units - chip_heads // group // 2], dq_sent.at[0])

        @pl.when(chip // (chips // 2) != core)
        def _():
            sent(dq_buf, dq_sent.at[0])

        for e in range(reach + 1):
            @pl.when(chip >= e)
            def _():
                kvg_copy(e).wait_send()

        for c in range(chips):
            @pl.when(chip == c)
            def _():
                if c < last:
                    sent(right_buf.at[c + 1:], right_sent.at[0])
                if c > 0:
                    sent(left_buf.at[:c], left_sent.at[0])

        @pl.when(sec > 0)
        def _():
            sent(final, final_sent.at[0])

        @pl.when(sec < sections - 1)
        def _():
            each(0, chunks, lambda k: final_copy(k).wait_recv())


def body(queries, keys, values, out_grad, documents, query_weight, key_weight, value_weight):
    sections = lax.axis_size("section")
    count = lax.axis_size("seq")
    tok = queries.shape[1]
    total = tok * count
    kv = keys.shape[2] // HD
    feats = query_weight.shape[1]
    heads = feats // HD
    width = query_weight.shape[2]
    chips = count // 2
    rows = 2 * tok
    reach = -(-(total // 2) // rows)
    group = 2
    cw = min(256, width)
    chunks = width // cw
    units = chips * heads // group
    kvh = kv // 2
    slots = (reach + 1) * rows
    dma = pltpu.SemaphoreType.DMA
    anywhere = pl.BlockSpec(memory_space=pl.ANY)
    vmem = pl.BlockSpec(memory_space=pltpu.VMEM)
    out = pl.pallas_call(
        functools.partial(kernel, (sections, count, tok, heads, kv, width, cw, group, reach)),
        out_shape=pltpu.VMEM((tok, width), BF16),
        in_specs=[anywhere] * 8,
        out_specs=vmem,
        scratch_shapes=[
            pltpu.VMEM((1, total), jnp.int32),
            pltpu.VMEM((rows, chips * feats), BF16),
            pltpu.VMEM((rows, chips * feats), BF16),
            pltpu.VMEM((2, tok, kv * HD), BF16),
            pltpu.VMEM((2, kvh, slots, HD), BF16),
            pltpu.VMEM((HD, slots), BF16),
            pltpu.VMEM((slots, rows), F32),
            pltpu.VMEM((slots, HD), F32),
            pltpu.VMEM((slots, HD), F32),
            pltpu.VMEM((units, rows, group * HD), BF16),
            pltpu.VMEM((chips, tok, 2 * feats), BF16),
            pltpu.VMEM((reach + 1, 2, tok, 2 * kv * HD), BF16),
            pltpu.VMEM((2 * feats, width), BF16),
            pltpu.VMEM((2 * kv * HD, width), BF16),
            pltpu.VMEM((chips, chunks, tok, cw), BF16),
            pltpu.VMEM((chips, chunks, tok, cw), BF16),
            pltpu.VMEM((tok, cw), F32),
            pltpu.VMEM((chunks, tok, cw), BF16),
            dma((1,)),
            dma((2,)),
            dma((2,)),
            dma((2, 2)),
            dma((1,)),
            dma((2, kvh, reach + 1)),
            dma((1,)),
            dma((5,)),
            dma((1,)),
            dma((1,)),
            dma((1,)),
            dma((chips,)),
            dma((reach + 1,)),
            dma((reach + 1,)),
            dma((1,)),
            dma((chips - 1, chunks)),
            dma((1,)),
            dma((chips - 1, chunks)),
            dma((1,)),
            dma((chunks,)),
        ],
        compiler_params=pltpu.CompilerParams(
            collective_id=0, has_side_effects=True, vmem_limit_bytes=60 * 1024 * 1024),
        name="attention_back",
    )(queries[0], keys[0], values[0], out_grad[0], documents,
      query_weight[0], key_weight[0], value_weight[0])
    return out[None]


def solution(mesh):
    in_specs = (
        P("section", "seq", None),
        P("section", "seq", None),
        P("section", "seq", None),
        P("section", "seq", None),
        P("section", None),
        P("section", "seq", None),
        P("section", None, None),
        P("section", None, None),
    )
    out_specs = P("section", "seq", None)
    return jax.shard_map(body, mesh=mesh, in_specs=in_specs, out_specs=out_specs, check_vma=False)
```

```python
import functools
import math

import jax
import jax.numpy as jnp
from jax import lax
from jax.experimental import pallas as pl
from jax.experimental.pallas import tpu as pltpu
from jax.sharding import PartitionSpec as P

HD = 128
MESH = pl.DeviceIdType.MESH
F32 = jnp.float32
BF16 = jnp.bfloat16


def aligned(index, size):
    return pl.ds(pl.multiple_of(index * size, size), size)


def kernel(dims, q_in, k_in, v_in, o_in, ids_in, wq_in, wk_in, wv_in, out_ref,
           ids_ref, q_all, o_all, kv_own_all, kv_all, k_turned, bias, dk_sum, dv_sum, dq_buf, grads, kv_grads,
           weights, kv_weights, right_buf, left_buf, acc, final,
           ids_got, stage_got, qo_sent, qo_got, kv_sent, kv_got, kv_passed, w_local, w_sent, w_got,
           dq_sent, g_got, kvg_sent, kvg_got,
           right_sent, right_got, left_sent, left_got, near_got, half_got, final_sent, final_got):
    sections, count, tok, heads, kv, width, cw, group, reach = dims
    chips = count // 2
    rows = 2 * tok
    feats = heads * HD
    chip_heads = 2 * heads
    own_heads = chips * heads
    units = own_heads // group
    half_feats = own_heads * HD
    kvh = kv // 2
    per = own_heads // kvh
    chunks = width // cw
    span = 2 * kvh * HD
    scale = 1.0 / math.sqrt(HD)
    to_log2 = scale * math.log2(math.e)
    sec = lax.axis_index("section")
    me = lax.axis_index("seq")
    chip = me // 2
    core = me % 2
    partner = (sec, me + 1 - 2 * core)
    last = chips - 1

    def remote(src, dst, send_sem, recv_sem, device):
        return pltpu.make_async_remote_copy(
            src_ref=src, dst_ref=dst, send_sem=send_sem, recv_sem=recv_sem,
            device_id=device, device_id_type=MESH)

    kv_in = (k_in, v_in)
    right = jnp.minimum(chip + 1, last)

    def kv_head(half, g):
        return pl.ds(pl.multiple_of((half * kvh + g) * HD, HD), HD)

    def kv_right(which, g, p):
        return remote(kv_own_all.at[which, :, kv_head(p, g)],
                      kv_all.at[which, g, pl.ds(pl.multiple_of((reach - 1) * rows + core * tok, tok), tok)],
                      kv_sent.at[0], kv_got.at[which, g, 1], (sec, 2 * right + p))

    def kv_direct(which, g, p):
        return remote(kv_own_all.at[which, :, kv_head(p, g)],
                      kv_all.at[which, g, pl.ds(pl.multiple_of((reach - 2) * rows + core * tok, tok), tok)],
                      kv_sent.at[0], kv_got.at[which, g, 2], (sec, 2 * last + p))

    def kv_partner(which, g):
        return remote(kv_own_all.at[which, :, kv_head(1 - core, g)],
                      kv_all.at[which, g, pl.ds(pl.multiple_of(reach * rows + core * tok, tok), tok)],
                      kv_sent.at[0], kv_got.at[which, g, 0], partner)

    def kv_own(which, g):
        return pltpu.make_async_copy(
            kv_in[which].at[:, kv_head(core, g)],
            kv_all.at[which, g, pl.ds(pl.multiple_of(reach * rows + core * tok, tok), tok)],
            kv_got.at[which, g, 0])

    def kv_block(which, g, e):
        return kv_all.at[which, g, pl.ds((reach - e) * rows, rows)]

    def kv_relay(which, g, e):
        return remote(kv_block(which, g, e), kv_block(which, g, e + 1),
                      kv_passed.at[0], kv_got.at[which, g, e + 1],
                      (sec, 2 * right + core))

    def kv_wait(which, g, e):
        part = kv_block(which, g, e)
        pltpu.make_async_copy(part, part, kv_got.at[which, g, e]).wait()

    def pass_kv(g, e):
        with jax.named_scope('relay'):
            for which in range(2):
                kv_wait(which, g, e)
                kv_relay(which, g, e).start()

    def qo_partner(which):
        return remote((q_in, o_in)[which].at[:, aligned(1 - core, half_feats)],
                      (q_all, o_all)[which].at[aligned(core, tok)],
                      qo_sent.at[which], qo_got.at[which], partner)

    def qo_own(which):
        return pltpu.make_async_copy((q_in, o_in)[which].at[:, aligned(core, half_feats)],
                                     (q_all, o_all)[which].at[aligned(core, tok)],
                                     qo_got.at[which])

    w_copy = remote(wq_in, weights.at[aligned(core, feats)], w_sent.at[0], w_got.at[0], partner)

    direct = reach > 1 and chips > 2

    def goes_on(g, e):
        return chip < (last - 1 if direct and g == 0 and e == 1 else last)

    def send_right(g):
        if direct and g == 0:
            @pl.when(chip == last - 2)
            def _():
                for p in range(2):
                    for which in range(2):
                        kv_direct(which, g, p).start()

        @pl.when(chip < last)
        def _():
            for p in range(2):
                for which in range(2):
                    kv_right(which, g, p).start()

    staged = [pltpu.make_async_copy(kv_in[which], kv_own_all.at[which], stage_got.at[which])
              for which in range(2)]
    ids_copy = pltpu.make_async_copy(ids_in, ids_ref, ids_got.at[0])
    for copy in staged + [ids_copy]:
        copy.start()
    for which in range(2):
        qo_own(which).start()
    for g in range(kvh):
        for which in range(2):
            kv_own(which, g).start()
    local = [pltpu.make_async_copy(wq_in, weights.at[aligned(core, feats)], w_local.at[0])]
    for r in range(2):
        part = slice(r * kvh * HD, (r + 1) * kvh * HD)
        for which, source in enumerate((wk_in, wv_in)):
            base = r * span + which * kvh * HD
            local.append(pltpu.make_async_copy(
                source.at[part], kv_weights.at[base:base + kvh * HD],
                w_local.at[1]))
    barrier = pltpu.get_barrier_semaphore()

    def greet(device):
        pl.semaphore_signal(barrier, inc=1, device_id=device, device_id_type=MESH)

    for off in range(1, count):
        greet((sec, lax.rem(me + off, count)))

    @pl.when(sec > 0)
    def _():
        greet((sec - 1, me))

    @pl.when(sec < sections - 1)
    def _():
        greet((sec + 1, me))

    above = jnp.where(sec > 0, 1, 0)
    below = jnp.where(sec < sections - 1, 1, 0)
    with jax.named_scope('barrier'):
        pl.semaphore_wait(barrier, count - 1 + above + below)

    for copy in staged:
        copy.wait()

    send_right(0)
    for g in range(1, kvh):
        send_right(g)

    for g in range(kvh):
        for which in range(2):
            kv_partner(which, g).start()
    for which in range(2):
        qo_partner(which).start()

    w_copy.start()
    for copy in local:
        copy.start()

    @pl.when(sec == sections - 1)
    def _():
        out_ref[...] = jnp.zeros_like(out_ref)

    ids_copy.wait()
    q_ids = ids_ref[:, aligned(chip, rows)]

    def set_bias(blocks):
        here = blocks * rows
        first = pl.ds(pl.multiple_of((chip + 1 - blocks) * rows, rows), here)
        k_ids = jnp.broadcast_to(ids_ref[:, first], (HD, here)).T[:, :1]
        same = k_ids == q_ids
        j = lax.broadcasted_iota(jnp.int32, (here, rows), 0)
        i = lax.broadcasted_iota(jnp.int32, (here, rows), 1) + (blocks - 1) * rows
        bias[:here] = jnp.where(same & (j <= i), 0.0, -jnp.inf)

    for blocks in range(1, reach + 2):
        @pl.when(jnp.minimum(chip, reach) + 1 == blocks)
        def _():
            with jax.named_scope('bias'):
                set_bias(blocks)

    for g in range(kvh):
        for e in range(1, reach):
            from_chip = e if g == 0 else max(e, 2)

            @pl.when((chip >= from_chip) & goes_on(g, e))
            def _():
                pass_kv(g, e)

    with jax.named_scope('qo_wait'):
        for which in range(2):
            buf = (q_all, o_all)[which]
            pltpu.make_async_copy(buf, buf, qo_got.at[which]).wait()

    def dq_place(unit):
        head = unit * group
        target = core * (chips // 2) + head // chip_heads
        piece = (head % chip_heads) // group
        return target, piece

    def dq_copy(unit, p):
        target, piece = dq_place(unit)
        return remote(dq_buf.at[unit, p * tok:(p + 1) * tok],
                      grads.at[chip, :, aligned(piece, group * HD)],
                      dq_sent.at[0], g_got.at[chip], (sec, 2 * target + p))

    def dq_out(unit, reaches=None):
        target, piece = dq_place(unit)
        for p in range(2):
            @pl.when((2 * target + p != me) if reaches is None else (2 * target + p != me) & (target <= reaches))
            def _():
                dq_copy(unit, p).start()

            @pl.when(2 * target + p == me)
            def _():
                grads[chip, :, aligned(piece, group * HD)] = dq_buf[unit, p * tok:(p + 1) * tok]

    dims_last = (((1,), (1,)), ((), ()))

    early = chunks * 3 // 16 * 2 if chips > 3 else 0
    early_left = chunks // 8 * 2 if chips > 3 else 0

    def far_out(first, end=chips):
        def far_unit(n, carry):
            unit = units - 1 - n
            target, _ = dq_place(unit)

            @pl.when((target >= first) & (target < end))
            def _():
                for p in range(2):
                    dq_copy(unit, p).start()

            return carry

        lax.fori_loop(0, units, far_unit, 0)

    held = min(2, reach)
    batch = 1

    def attend(blocks):
        here = blocks * rows
        low = (reach + 1 - blocks) * rows
        for turn in range(kvh):
            g = jnp.where(core == 0, kvh - 1 - turn, turn) if blocks == 1 else turn
            with jax.named_scope('kv_wait'):
                for e in range(blocks):
                    if 1 <= e < reach:
                        @pl.when(~goes_on(g, e))
                        def _():
                            kv_wait(0, g, e)
                            kv_wait(1, g, e)
                    else:
                        kv_wait(0, g, e)
                        kv_wait(1, g, e)
            k_turned[:, :here] = kv_all[0, g, low:].T
            dk_sum[:here] = jnp.zeros((here, HD), F32)
            dv_sum[:here] = jnp.zeros((here, HD), F32)

            def unit_of(n, h):
                return g * (per // group) + n * batch + h // group

            def one_batch(n, carry):
                dk = jnp.zeros((here, HD), F32)
                dv = jnp.zeros((here, HD), F32)
                heads_here = range(batch * group)
                cols = [aligned(unit_of(n, h) * group + h % group, HD) for h in heads_here]
                scores, dprobs = {}, {}

                def start_head(h):
                    scores[h] = lax.dot_general(kv_all[0, g, low:], q_all[:, cols[h]], dims_last,
                                                preferred_element_type=F32) + bias[:here]
                    dprobs[h] = lax.dot_general(kv_all[1, g, low:], o_all[:, cols[h]], dims_last,
                                                preferred_element_type=F32)

                def weigh(h):
                    s, dp = scores.pop(h), dprobs.pop(h)
                    top = jnp.max(s, axis=0, keepdims=True)
                    e = jnp.exp2((s - top) * to_log2)
                    inv = 1.0 / jnp.sum(e, axis=0, keepdims=True)
                    delta = jnp.sum(e * dp, axis=0, keepdims=True) * inv
                    prob = e * inv
                    return prob.astype(BF16), (prob * (dp - delta)).astype(BF16)

                start_head(0)
                for h in heads_here:
                    if h + 1 < len(heads_here):
                        start_head(h + 1)
                    prob, ds = weigh(h)
                    dv += jnp.dot(prob, o_all[:, cols[h]], preferred_element_type=F32)
                    dk += jnp.dot(ds, q_all[:, cols[h]], preferred_element_type=F32)
                    dq = jnp.dot(k_turned[:, :here], ds, preferred_element_type=F32) * scale
                    at = h % group
                    dq_buf[unit_of(n, h), :, at * HD:(at + 1) * HD] = dq.T.astype(BF16)
                if at == group - 1:
                        dq_out(unit_of(n, h), 1 if blocks <= held else None)
                dk_sum[:here] += dk
                dv_sum[:here] += dv
                if blocks == 2 and reach > 1 and turn + 1 < kvh:
                    @pl.when((n == per // group // batch // 2 - 1) & goes_on(turn + 1, 1))
                    def _():
                        pass_kv(turn + 1, 1)

                return carry

            with jax.named_scope('attend'):
                lax.fori_loop(0, per // group // batch, one_batch, 0)
            for e in range(blocks):
                at = (blocks - 1 - e) * rows
                for which, sums in enumerate((dk_sum, dv_sum)):
                    col = aligned(core * 2 * kvh + which * kvh + g, HD)
                    for p in range(2):
                        part = sums[at + p * tok:at + (p + 1) * tok]
                        if which == 0:
                            part = part * scale
                        kv_grads[e, p, :, col] = part.astype(BF16)

        if blocks <= held:
            far_out(chips // 2 + 1 if blocks == 1 and early else 2)

    def kvg_copy(e):
        part = kv_grads.at[e, 1 - core, :, aligned(core, span)]
        return remote(part, part, kvg_sent.at[e], kvg_got.at[e], partner)

    for blocks in range(1, reach + 2):
        @pl.when(jnp.minimum(chip, reach) + 1 == blocks)
        def _():
            attend(blocks)
            for e in range(blocks):
                kvg_copy(e).start()

    def kvg_wait(e):
        with jax.named_scope('kvg_wait'):
            part = kv_grads.at[e, core, :, aligned(1 - core, span)]
            pltpu.make_async_copy(part, part, kvg_got.at[e]).wait()

    with jax.named_scope('w_wait'):
        local[0].wait()
        pltpu.make_async_copy(kv_weights, kv_weights, w_local.at[1]).wait()
        theirs = weights.at[aligned(1 - core, feats)]
        pltpu.make_async_copy(theirs, theirs, w_got.at[0]).wait()

    def grads_wait(b):
        with jax.named_scope('g_wait'):
            pltpu.make_async_copy(grads.at[b], grads.at[b], g_got.at[b]).wait()

    tail = chunks - 1
    half = cw // 2

    def right_target(section):
        return (section, jnp.minimum(me + 2, count - 2 + core))

    def left_target(section):
        return (section, jnp.maximum(me - 2, core))

    def start_one(buf, sent_sem, sem, d, k, target, beside):
        if d != beside:
            here = buf.at[d, k]
            remote(here, here, sent_sem.at[0], sem(d, k), target).start()
            return

        @pl.when(k < tail)
        def _():
            here = buf.at[d, k]
            remote(here, here, sent_sem.at[0], near_got.at[k], target).start()

        @pl.when(k == tail)
        def _():
            for h in range(2):
                here = buf.at[d, tail, :, h * half:(h + 1) * half]
                remote(here, here, sent_sem.at[0], half_got.at[0] if h else near_got.at[tail], target).start()

    def right_sem(d, k):
        return right_got.at[d - 2, k]

    def left_sem(d, k):
        return left_got.at[d, k]

    def got(part, sem):
        pltpu.make_async_copy(part, part, sem).wait()

    before = jnp.maximum(sec - 1, 0)
    is_beside = (chip == 1) | (chip == chips - 2)

    def final_copy(k):
        return remote(final.at[k], out_ref.at[:, aligned(k, cw)], final_sent.at[0], final_got.at[0],
                      (before, me))

    def final_half(h):
        return remote(final.at[tail, :, h * half:(h + 1) * half],
                      out_ref.at[:, tail * cw + h * half:tail * cw + (h + 1) * half],
                      final_sent.at[0], final_got.at[0], (before, me))

    def product(d, k):
        acc[...] = jnp.dot(grads[d], weights[:, aligned(k, cw)], preferred_element_type=F32)

    def kv_product(e, k):
        acc[...] += jnp.dot(kv_grads[e, core], kv_weights[:, aligned(k, cw)],
                            preferred_element_type=F32)

    def pass_right(d, k):
        with jax.named_scope('r_prod'):
            product(d, k)

        if d > 1:
            @pl.when(chip > 0)
            def _():
                with jax.named_scope('r_wait'):
                    got(right_buf.at[d, k], right_sem(d, k))
                acc[...] += right_buf[d, k].astype(F32)

        right_buf[d, k] = acc[...].astype(BF16)
        start_one(right_buf, right_sent, right_sem, d, k, right_target(sec), 1)

    def pass_left(d, k):
        with jax.named_scope('l_prod'):
            product(d, k)

            @pl.when(chip - d <= reach)
            def _():
                kv_product(jnp.minimum(chip - d, reach), k)

        if d < chips - 2:
            @pl.when(chip < last)
            def _():
                with jax.named_scope('l_wait'):
                    got(left_buf.at[d, k], left_sem(d, k))
                acc[...] += left_buf[d, k].astype(F32)

        left_buf[d, k] = acc[...].astype(BF16)
        start_one(left_buf, left_sent, left_sem, d, k, left_target(sec), chips - 2)

    def finish(k):
        with jax.named_scope('f_prod'):
            product(chip, k)
            kv_product(0, k)

        @pl.when(chip > 1)
        def _():
            with jax.named_scope('f_wait_r'):
                got(right_buf.at[chip, k], right_sem(chip, k))
            acc[...] += right_buf[chip, k].astype(F32)

        @pl.when(chip < chips - 2)
        def _():
            with jax.named_scope('f_wait_l'):
                got(left_buf.at[chip, k], left_sem(chip, k))
            acc[...] += left_buf[chip, k].astype(F32)

        for beside, buf in ((1, right_buf), (chips - 2, left_buf)):
            @pl.when((chip == beside) & (k < tail))
            def _():
                with jax.named_scope('f_wait_n'):
                    got(buf.at[beside, k], near_got.at[k])
                acc[...] += buf[beside, k].astype(F32)

        @pl.when(~is_beside | (k < tail))
        def _():
            final[k] = acc[...].astype(BF16)

            @pl.when(sec > 0)
            def _():
                final_copy(k).start()

        @pl.when(is_beside & (k == tail))
        def _():
            for h in range(2):
                cols = slice(h * half, (h + 1) * half)
                for beside, buf in ((1, right_buf), (chips - 2, left_buf)):
                    @pl.when(chip == beside)
                    def _():
                        got(buf.at[beside, tail, :, cols], half_got.at[0] if h else near_got.at[tail])
                        acc[:, cols] += buf[beside, tail, :, cols].astype(F32)

                final[tail, :, cols] = acc[:, cols].astype(BF16)

                @pl.when(sec > 0)
                def _():
                    final_half(h).start()

    def each(first, end, act):
        def one(k, carry):
            act(k)
            return carry

        lax.fori_loop(first, end, one, 0)

    lag = 4
    leads_right = chip < chips // 2

    if early:
        @pl.when(chip == 0)
        def _():
            grads_wait(1)
            far_out(2, chips // 2 + 1)
            each(0, early, lambda k: pass_right(1, k))

    for i in range(chips - 1):
        far, near = chips - 1 - i, i
        to_right = chip < far
        to_left = chip > near
        begin = early if i == chips - 2 else 0
        begin_left = early_left if i == chips - 2 else 0

        if early_left and i == chips - 3:
            @pl.when(chip == last)
            def _():
                grads_wait(chips - 2)
                kvg_wait(1)
                each(0, early_left, lambda k: pass_left(chips - 2, k))

        @pl.when(to_right)
        def _():
            if begin == 0:
                grads_wait(far)

        if begin_left == 0:
            @pl.when(to_left)
            def _():
                grads_wait(near)

            for e in range(1, reach + 1):
                @pl.when(chip == near + e)
                def _():
                    kvg_wait(e)

        if i == min(1, chips - 2):
            kvg_wait(0)
            for b in range(chips):
                @pl.when((chip == b) & (b // (chips // 2) != core))
                def _():
                    grads_wait(b)

        def one(step):
            k_right = step - jnp.where(leads_right, 0, lag)
            k_left = step - jnp.where(leads_right, lag, 0)

            @pl.when(to_right & (k_right >= begin) & (k_right < chunks))
            def _():
                pass_right(far, k_right)

            @pl.when(to_left & (k_left >= begin_left) & (k_left < chunks))
            def _():
                pass_left(near, k_left)

            if i == 1 and early:
                @pl.when((chip == 1) & (k_left >= 0) & (k_left < early))
                def _():
                    finish(k_left)

            if early_left and i == chips - 3:
                @pl.when((chip == chips - 2) & (k_right >= 0) & (k_right < early_left))
                def _():
                    finish(k_right)

        each(0, chunks + lag, one)

    done = jnp.where(chip == chips - 2, early_left, 0)
    each(jnp.where(chip == 1, early, done), chunks, finish)

    def sent(part, sem):
        pltpu.make_async_copy(part, part, sem).wait()

    with jax.named_scope('drain'):
        for c in range(chips):
            @pl.when(chip == c)
            def _():
                pieces = kvh * ((2 if c < last else 0) + 1) + (2 if direct and c == last - 2 else 0)
                sent(q_all.at[:, :pieces * HD], kv_sent.at[0])
                relays = kvh * min(c, reach - 1) if c < last else 0
                relays -= 1 if direct and c == last - 1 else 0
                if relays:
                    sent(q_all.at[:, :2 * relays * HD], kv_passed.at[0])

        for which in range(2):
            qo_partner(which).wait_send()
        w_copy.wait_send()

        @pl.when(chip // (chips // 2) == core)
        def _():
            sent(dq_buf.at[:units - chip_heads // group // 2], dq_sent.at[0])

        @pl.when(chip // (chips // 2) != core)
        def _():
            sent(dq_buf, dq_sent.at[0])

        for e in range(reach + 1):
            @pl.when(chip >= e)
            def _():
                kvg_copy(e).wait_send()

        for c in range(chips):
            @pl.when(chip == c)
            def _():
                if c < last:
                    sent(right_buf.at[c + 1:], right_sent.at[0])
                if c > 0:
                    sent(left_buf.at[:c], left_sent.at[0])

        @pl.when(sec > 0)
        def _():
            sent(final, final_sent.at[0])

        @pl.when(sec < sections - 1)
        def _():
            got(final, final_got.at[0])


def body(queries, keys, values, out_grad, documents, query_weight, key_weight, value_weight):
    sections = lax.axis_size("section")
    count = lax.axis_size("seq")
    tok = queries.shape[1]
    total = tok * count
    kv = keys.shape[2] // HD
    feats = query_weight.shape[1]
    heads = feats // HD
    width = query_weight.shape[2]
    chips = count // 2
    rows = 2 * tok
    reach = -(-(total // 2) // rows)
    group = 2
    cw = min(256, width)
    chunks = width // cw
    units = chips * heads // group
    kvh = kv // 2
    slots = (reach + 1) * rows
    dma = pltpu.SemaphoreType.DMA
    anywhere = pl.BlockSpec(memory_space=pl.ANY)
    vmem = pl.BlockSpec(memory_space=pltpu.VMEM)
    out = pl.pallas_call(
        functools.partial(kernel, (sections, count, tok, heads, kv, width, cw, group, reach)),
        out_shape=pltpu.VMEM((tok, width), BF16),
        in_specs=[anywhere] * 8,
        out_specs=vmem,
        scratch_shapes=[
            pltpu.VMEM((1, total), jnp.int32),
            pltpu.VMEM((rows, chips * feats), BF16),
            pltpu.VMEM((rows, chips * feats), BF16),
            pltpu.VMEM((2, tok, kv * HD), BF16),
            pltpu.VMEM((2, kvh, slots, HD), BF16),
            pltpu.VMEM((HD, slots), BF16),
            pltpu.VMEM((slots, rows), F32),
            pltpu.VMEM((slots, HD), F32),
            pltpu.VMEM((slots, HD), F32),
            pltpu.VMEM((units, rows, group * HD), BF16),
            pltpu.VMEM((chips, tok, 2 * feats), BF16),
            pltpu.VMEM((reach + 1, 2, tok, 2 * kv * HD), BF16),
            pltpu.VMEM((2 * feats, width), BF16),
            pltpu.VMEM((2 * kv * HD, width), BF16),
            pltpu.VMEM((chips, chunks, tok, cw), BF16),
            pltpu.VMEM((chips, chunks, tok, cw), BF16),
            pltpu.VMEM((tok, cw), F32),
            pltpu.VMEM((chunks, tok, cw), BF16),
            dma((1,)),
            dma((2,)),
            dma((2,)),
            dma((2,)),
            dma((1,)),
            dma((2, kvh, reach + 1)),
            dma((1,)),
            dma((2,)),
            dma((1,)),
            dma((1,)),
            dma((1,)),
            dma((chips,)),
            dma((reach + 1,)),
            dma((reach + 1,)),
            dma((1,)),
            dma((max(chips - 2, 1), chunks)),
            dma((1,)),
            dma((max(chips - 2, 1), chunks)),
            dma((chunks,)),
            dma((1,)),
            dma((1,)),
            dma((1,)),
        ],
        compiler_params=pltpu.CompilerParams(
            collective_id=0, has_side_effects=True, vmem_limit_bytes=60 * 1024 * 1024),
        name="attention_back",
    )(queries[0], keys[0], values[0], out_grad[0], documents,
      query_weight[0], key_weight[0], value_weight[0])
    return out[None]


def solution(mesh):
    in_specs = (
        P("section", "seq", None),
        P("section", "seq", None),
        P("section", "seq", None),
        P("section", "seq", None),
        P("section", None),
        P("section", "seq", None),
        P("section", None, None),
        P("section", None, None),
    )
    out_specs = P("section", "seq", None)
    return jax.shard_map(body, mesh=mesh, in_specs=in_specs, out_specs=out_specs, check_vma=False)
```

```python
import functools
import math

import jax
import jax.numpy as jnp
from jax import lax
from jax.experimental import pallas as pl
from jax.experimental.pallas import tpu as pltpu
from jax.sharding import PartitionSpec as P

HD = 128
MESH = pl.DeviceIdType.MESH
F32 = jnp.float32
BF16 = jnp.bfloat16


def aligned(index, size):
    return pl.ds(pl.multiple_of(index * size, size), size)


def kernel(dims, q_in, k_in, v_in, o_in, ids_in, wq_in, wk_in, wv_in, out_ref,
           ids_ref, q_all, o_all, kv_own_all, kv_all, k_turned, bias, dk_sum, dv_sum, dq_buf, grads, kv_grads,
           weights, kv_weights, right_buf, left_buf, acc, final,
           ids_got, stage_got, qo_sent, qo_got, kv_sent, kv_got, kv_passed, w_local, w_sent, w_got,
           dq_sent, g_got, kvg_sent, kvg_got,
           right_sent, right_got, left_sent, left_got, near_got, half_got, final_sent, final_got):
    sections, count, tok, heads, kv, width, cw, group, reach = dims
    chips = count // 2
    rows = 2 * tok
    feats = heads * HD
    chip_heads = 2 * heads
    own_heads = chips * heads
    units = own_heads // group
    half_feats = own_heads * HD
    kvh = kv // 2
    per = own_heads // kvh
    chunks = width // cw
    span = 2 * kvh * HD
    scale = 1.0 / math.sqrt(HD)
    to_log2 = scale * math.log2(math.e)
    sec = lax.axis_index("section")
    me = lax.axis_index("seq")
    chip = me // 2
    core = me % 2
    partner = (sec, me + 1 - 2 * core)
    last = chips - 1

    def remote(src, dst, send_sem, recv_sem, device):
        return pltpu.make_async_remote_copy(
            src_ref=src, dst_ref=dst, send_sem=send_sem, recv_sem=recv_sem,
            device_id=device, device_id_type=MESH)

    kv_in = (k_in, v_in)
    right = jnp.minimum(chip + 1, last)

    def kv_head(half, g):
        return pl.ds(pl.multiple_of((half * kvh + g) * HD, HD), HD)

    def kv_right(which, g, p):
        return remote(kv_own_all.at[which, :, kv_head(p, g)],
                      kv_all.at[which, g, pl.ds(pl.multiple_of((reach - 1) * rows + core * tok, tok), tok)],
                      kv_sent.at[0], kv_got.at[which, g, 1], (sec, 2 * right + p))

    def kv_direct(which, g, p):
        return remote(kv_own_all.at[which, :, kv_head(p, g)],
                      kv_all.at[which, g, pl.ds(pl.multiple_of((reach - 2) * rows + core * tok, tok), tok)],
                      kv_sent.at[0], kv_got.at[which, g, 2], (sec, 2 * last + p))

    def kv_partner(which, g):
        return remote(kv_own_all.at[which, :, kv_head(1 - core, g)],
                      kv_all.at[which, g, pl.ds(pl.multiple_of(reach * rows + core * tok, tok), tok)],
                      kv_sent.at[0], kv_got.at[which, g, 0], partner)

    def kv_own(which, g):
        return pltpu.make_async_copy(
            kv_in[which].at[:, kv_head(core, g)],
            kv_all.at[which, g, pl.ds(pl.multiple_of(reach * rows + core * tok, tok), tok)],
            kv_got.at[which, g, 0])

    def kv_block(which, g, e):
        return kv_all.at[which, g, pl.ds((reach - e) * rows, rows)]

    def kv_relay(which, g, e):
        return remote(kv_block(which, g, e), kv_block(which, g, e + 1),
                      kv_passed.at[0], kv_got.at[which, g, e + 1],
                      (sec, 2 * right + core))

    def kv_wait(which, g, e):
        part = kv_block(which, g, e)
        pltpu.make_async_copy(part, part, kv_got.at[which, g, e]).wait()

    def pass_kv(g, e):
        with jax.named_scope('relay'):
            for which in range(2):
                kv_wait(which, g, e)
                kv_relay(which, g, e).start()

    def qo_partner(which):
        return remote((q_in, o_in)[which].at[:, aligned(1 - core, half_feats)],
                      (q_all, o_all)[which].at[aligned(core, tok)],
                      qo_sent.at[which], qo_got.at[which], partner)

    def qo_own(which):
        return pltpu.make_async_copy((q_in, o_in)[which].at[:, aligned(core, half_feats)],
                                     (q_all, o_all)[which].at[aligned(core, tok)],
                                     qo_got.at[which])

    w_copy = remote(wq_in, weights.at[aligned(core, feats)], w_sent.at[0], w_got.at[0], partner)

    direct = reach > 1 and chips > 2

    def goes_on(g, e):
        return chip < (last - 1 if direct and g == 0 and e == 1 else last)

    def send_right(g):
        if direct and g == 0:
            @pl.when(chip == last - 2)
            def _():
                for p in range(2):
                    for which in range(2):
                        kv_direct(which, g, p).start()

        @pl.when(chip < last)
        def _():
            for p in range(2):
                for which in range(2):
                    kv_right(which, g, p).start()

    staged = [pltpu.make_async_copy(kv_in[which], kv_own_all.at[which], stage_got.at[which])
              for which in range(2)]
    ids_copy = pltpu.make_async_copy(ids_in, ids_ref, ids_got.at[0])
    for copy in staged + [ids_copy]:
        copy.start()
    for which in range(2):
        qo_own(which).start()
    for g in range(kvh):
        for which in range(2):
            kv_own(which, g).start()
    local = [pltpu.make_async_copy(wq_in, weights.at[aligned(core, feats)], w_local.at[0])]
    for r in range(2):
        part = slice(r * kvh * HD, (r + 1) * kvh * HD)
        for which, source in enumerate((wk_in, wv_in)):
            base = r * span + which * kvh * HD
            local.append(pltpu.make_async_copy(
                source.at[part], kv_weights.at[base:base + kvh * HD],
                w_local.at[1]))
    barrier = pltpu.get_barrier_semaphore()

    def greet(device):
        pl.semaphore_signal(barrier, inc=1, device_id=device, device_id_type=MESH)

    for off in range(1, count):
        greet((sec, lax.rem(me + off, count)))

    @pl.when(sec > 0)
    def _():
        greet((sec - 1, me))

    @pl.when(sec < sections - 1)
    def _():
        greet((sec + 1, me))

    above = jnp.where(sec > 0, 1, 0)
    below = jnp.where(sec < sections - 1, 1, 0)
    with jax.named_scope('barrier'):
        pl.semaphore_wait(barrier, count - 1 + above + below)

    for copy in staged:
        copy.wait()

    send_right(0)
    for g in range(1, kvh):
        send_right(g)

    for g in range(kvh):
        for which in range(2):
            kv_partner(which, g).start()
    for which in range(2):
        qo_partner(which).start()

    w_copy.start()
    for copy in local:
        copy.start()

    ids_copy.wait()
    q_ids = ids_ref[:, aligned(chip, rows)]

    def set_bias(blocks):
        here = blocks * rows
        first = pl.ds(pl.multiple_of((chip + 1 - blocks) * rows, rows), here)
        k_ids = jnp.broadcast_to(ids_ref[:, first], (HD, here)).T[:, :1]
        same = k_ids == q_ids
        j = lax.broadcasted_iota(jnp.int32, (here, rows), 0)
        i = lax.broadcasted_iota(jnp.int32, (here, rows), 1) + (blocks - 1) * rows
        bias[:here] = jnp.where(same & (j <= i), 0.0, -jnp.inf)

    for blocks in range(1, reach + 2):
        @pl.when(jnp.minimum(chip, reach) + 1 == blocks)
        def _():
            with jax.named_scope('bias'):
                set_bias(blocks)

    for g in range(kvh):
        for e in range(1, reach):
            from_chip = e if g == 0 else max(e, 2)

            @pl.when((chip >= from_chip) & goes_on(g, e))
            def _():
                pass_kv(g, e)

    with jax.named_scope('qo_wait'):
        for which in range(2):
            buf = (q_all, o_all)[which]
            pltpu.make_async_copy(buf, buf, qo_got.at[which]).wait()

    def dq_place(unit):
        head = unit * group
        target = core * (chips // 2) + head // chip_heads
        piece = (head % chip_heads) // group
        return target, piece

    def dq_copy(unit, p):
        target, piece = dq_place(unit)
        return remote(dq_buf.at[unit, p * tok:(p + 1) * tok],
                      grads.at[chip, :, aligned(piece, group * HD)],
                      dq_sent.at[0], g_got.at[chip], (sec, 2 * target + p))

    def dq_out(unit, reaches=None):
        target, piece = dq_place(unit)
        for p in range(2):
            @pl.when((2 * target + p != me) if reaches is None else (2 * target + p != me) & (target <= reaches))
            def _():
                dq_copy(unit, p).start()

            @pl.when(2 * target + p == me)
            def _():
                grads[chip, :, aligned(piece, group * HD)] = dq_buf[unit, p * tok:(p + 1) * tok]

    dims_last = (((1,), (1,)), ((), ()))

    early = chunks * 3 // 16 * 2 if chips > 3 else 0
    early_left = chunks // 2 if chips > 3 else 0

    def far_out(first, end=chips):
        def far_unit(n, carry):
            unit = units - 1 - n
            target, _ = dq_place(unit)

            @pl.when((target >= first) & (target < end))
            def _():
                for p in range(2):
                    dq_copy(unit, p).start()

            return carry

        lax.fori_loop(0, units, far_unit, 0)

    held = min(2, reach)
    batch = 1

    def attend(blocks):
        here = blocks * rows
        low = (reach + 1 - blocks) * rows
        for turn in range(kvh):
            g = jnp.where(core == 0, kvh - 1 - turn, turn) if blocks == 1 else turn
            with jax.named_scope('kv_wait'):
                for e in range(blocks):
                    if 1 <= e < reach:
                        @pl.when(~goes_on(g, e))
                        def _():
                            kv_wait(0, g, e)
                            kv_wait(1, g, e)
                    else:
                        kv_wait(0, g, e)
                        kv_wait(1, g, e)
            k_turned[:, :here] = kv_all[0, g, low:].T
            dk_sum[:here] = jnp.zeros((here, HD), F32)
            dv_sum[:here] = jnp.zeros((here, HD), F32)

            def unit_of(n, h):
                return g * (per // group) + n * batch + h // group

            def one_batch(n, carry):
                dk = jnp.zeros((here, HD), F32)
                dv = jnp.zeros((here, HD), F32)
                heads_here = range(batch * group)
                cols = [aligned(unit_of(n, h) * group + h % group, HD) for h in heads_here]
                scores, dprobs = {}, {}

                def start_head(h):
                    scores[h] = lax.dot_general(kv_all[0, g, low:], q_all[:, cols[h]], dims_last,
                                                preferred_element_type=F32) + bias[:here]
                    dprobs[h] = lax.dot_general(kv_all[1, g, low:], o_all[:, cols[h]], dims_last,
                                                preferred_element_type=F32)

                def weigh(h):
                    s, dp = scores.pop(h), dprobs.pop(h)
                    top = jnp.max(s, axis=0, keepdims=True)
                    e = jnp.exp2((s - top) * to_log2)
                    inv = 1.0 / jnp.sum(e, axis=0, keepdims=True)
                    delta = jnp.sum(e * dp, axis=0, keepdims=True) * inv
                    prob = e * inv
                    return prob.astype(BF16), (prob * (dp - delta)).astype(BF16)

                start_head(0)
                for h in heads_here:
                    if h + 1 < len(heads_here):
                        start_head(h + 1)
                    prob, ds = weigh(h)
                    dv += jnp.dot(prob, o_all[:, cols[h]], preferred_element_type=F32)
                    dk += jnp.dot(ds, q_all[:, cols[h]], preferred_element_type=F32)
                    dq = jnp.dot(k_turned[:, :here], ds, preferred_element_type=F32) * scale
                    at = h % group
                    dq_buf[unit_of(n, h), :, at * HD:(at + 1) * HD] = dq.T.astype(BF16)
                dq_out(unit_of(n, 0), 1 if blocks <= held else None)
                dk_sum[:here] += dk
                dv_sum[:here] += dv
                if blocks == 2 and reach > 1 and turn + 1 < kvh:
                    @pl.when((n == per // group // batch // 2 - 1) & goes_on(turn + 1, 1))
                    def _():
                        pass_kv(turn + 1, 1)

                return carry

            with jax.named_scope('attend'):
                lax.fori_loop(0, per // group // batch, one_batch, 0)
            for e in range(blocks):
                at = (blocks - 1 - e) * rows
                for which, sums in enumerate((dk_sum, dv_sum)):
                    col = aligned(core * 2 * kvh + which * kvh + g, HD)
                    for p in range(2):
                        part = sums[at + p * tok:at + (p + 1) * tok]
                        if which == 0:
                            part = part * scale
                        kv_grads[e, p, :, col] = part.astype(BF16)

        if blocks <= held:
            far_out(chips // 2 + 1 if blocks == 1 and early else 2)

    def kvg_copy(e):
        part = kv_grads.at[e, 1 - core, :, aligned(core, span)]
        return remote(part, part, kvg_sent.at[e], kvg_got.at[e], partner)

    for blocks in range(1, reach + 2):
        @pl.when(jnp.minimum(chip, reach) + 1 == blocks)
        def _():
            attend(blocks)
            for e in range(blocks):
                kvg_copy(e).start()

    def kvg_wait(e):
        with jax.named_scope('kvg_wait'):
            part = kv_grads.at[e, core, :, aligned(1 - core, span)]
            pltpu.make_async_copy(part, part, kvg_got.at[e]).wait()

    with jax.named_scope('w_wait'):
        local[0].wait()
        pltpu.make_async_copy(kv_weights, kv_weights, w_local.at[1]).wait()
        theirs = weights.at[aligned(1 - core, feats)]
        pltpu.make_async_copy(theirs, theirs, w_got.at[0]).wait()

    def grads_wait(b):
        with jax.named_scope('g_wait'):
            pltpu.make_async_copy(grads.at[b], grads.at[b], g_got.at[b]).wait()

    tail = chunks - 1
    half = cw // 2

    def right_target(section):
        return (section, jnp.minimum(me + 2, count - 2 + core))

    def left_target(section):
        return (section, jnp.maximum(me - 2, core))

    def start_one(buf, sent_sem, sem, d, k, target, beside):
        if d != beside:
            here = buf.at[d, k]
            remote(here, here, sent_sem.at[0], sem(d, k), target).start()
            return

        @pl.when(k < tail)
        def _():
            here = buf.at[d, k]
            remote(here, here, sent_sem.at[0], near_got.at[k], target).start()

        @pl.when(k == tail)
        def _():
            for h in range(2):
                here = buf.at[d, tail, :, h * half:(h + 1) * half]
                remote(here, here, sent_sem.at[0], half_got.at[0] if h else near_got.at[tail], target).start()

    def right_sem(d, k):
        return right_got.at[d - 2, k]

    def left_sem(d, k):
        return left_got.at[d, k]

    def got(part, sem):
        pltpu.make_async_copy(part, part, sem).wait()

    before = jnp.maximum(sec - 1, 0)
    is_beside = (chip == 1) | (chip == chips - 2)

    def final_copy(k):
        return remote(final.at[k], out_ref.at[:, aligned(k, cw)], final_sent.at[0], final_got.at[0],
                      (before, me))

    def final_half(h):
        return remote(final.at[tail, :, h * half:(h + 1) * half],
                      out_ref.at[:, tail * cw + h * half:tail * cw + (h + 1) * half],
                      final_sent.at[0], final_got.at[0], (before, me))

    def product(d, k):
        acc[...] = jnp.dot(grads[d], weights[:, aligned(k, cw)], preferred_element_type=F32)

    def kv_product(e, k):
        acc[...] += jnp.dot(kv_grads[e, core], kv_weights[:, aligned(k, cw)],
                            preferred_element_type=F32)

    def pass_right(d, k):
        with jax.named_scope('r_prod'):
            product(d, k)

        if d > 1:
            @pl.when(chip > 0)
            def _():
                with jax.named_scope('r_wait'):
                    got(right_buf.at[d, k], right_sem(d, k))
                acc[...] += right_buf[d, k].astype(F32)

        right_buf[d, k] = acc[...].astype(BF16)
        start_one(right_buf, right_sent, right_sem, d, k, right_target(sec), 1)

    def pass_left(d, k):
        with jax.named_scope('l_prod'):
            product(d, k)

            @pl.when(chip - d <= reach)
            def _():
                kv_product(jnp.minimum(chip - d, reach), k)

        if d < chips - 2:
            @pl.when(chip < last)
            def _():
                with jax.named_scope('l_wait'):
                    got(left_buf.at[d, k], left_sem(d, k))
                acc[...] += left_buf[d, k].astype(F32)

        left_buf[d, k] = acc[...].astype(BF16)
        start_one(left_buf, left_sent, left_sem, d, k, left_target(sec), chips - 2)

    def finish(k):
        with jax.named_scope('f_prod'):
            product(chip, k)
            kv_product(0, k)

        @pl.when(chip > 1)
        def _():
            with jax.named_scope('f_wait_r'):
                got(right_buf.at[chip, k], right_sem(chip, k))
            acc[...] += right_buf[chip, k].astype(F32)

        @pl.when(chip < chips - 2)
        def _():
            with jax.named_scope('f_wait_l'):
                got(left_buf.at[chip, k], left_sem(chip, k))
            acc[...] += left_buf[chip, k].astype(F32)

        for beside, buf in ((1, right_buf), (chips - 2, left_buf)):
            @pl.when((chip == beside) & (k < tail))
            def _():
                with jax.named_scope('f_wait_n'):
                    got(buf.at[beside, k], near_got.at[k])
                acc[...] += buf[beside, k].astype(F32)

        @pl.when(~is_beside | (k < tail))
        def _():
            final[k] = acc[...].astype(BF16)

            @pl.when(sec > 0)
            def _():
                final_copy(k).start()

        @pl.when(is_beside & (k == tail))
        def _():
            for h in range(2):
                cols = slice(h * half, (h + 1) * half)
                for beside, buf in ((1, right_buf), (chips - 2, left_buf)):
                    @pl.when(chip == beside)
                    def _():
                        got(buf.at[beside, tail, :, cols], half_got.at[0] if h else near_got.at[tail])
                        acc[:, cols] += buf[beside, tail, :, cols].astype(F32)

                final[tail, :, cols] = acc[:, cols].astype(BF16)

                @pl.when(sec > 0)
                def _():
                    final_half(h).start()

    def each(first, end, act):
        def one(k, carry):
            act(k)
            return carry

        lax.fori_loop(first, end, one, 0)

    lag = 4
    leads_right = chip < chips // 2

    if early:
        @pl.when(chip == 0)
        def _():
            grads_wait(1)
            far_out(2, chips // 2 + 1)
            each(0, early, lambda k: pass_right(1, k))

    for i in range(chips - 1):
        far, near = chips - 1 - i, i
        to_right = chip < far
        to_left = chip > near
        begin = early if i == chips - 2 else 0
        begin_left = early_left if i == chips - 2 else 0

        if early_left and i == chips - 3:
            @pl.when(chip == last)
            def _():
                grads_wait(chips - 2)
                kvg_wait(1)
                each(0, early_left, lambda k: pass_left(chips - 2, k))

        @pl.when(to_right)
        def _():
            if begin == 0:
                grads_wait(far)

        if begin_left == 0:
            @pl.when(to_left)
            def _():
                grads_wait(near)

            for e in range(1, reach + 1):
                @pl.when(chip == near + e)
                def _():
                    kvg_wait(e)

        if i == min(1, chips - 2):
            kvg_wait(0)
            for b in range(chips):
                @pl.when((chip == b) & (b // (chips // 2) != core))
                def _():
                    grads_wait(b)

        def one(step):
            k_right = step - jnp.where(leads_right, 0, lag)
            k_left = step - jnp.where(leads_right, lag, 0)

            @pl.when(to_right & (k_right >= begin) & (k_right < chunks))
            def _():
                pass_right(far, k_right)

            @pl.when(to_left & (k_left >= begin_left) & (k_left < chunks))
            def _():
                pass_left(near, k_left)

            if i == 1 and early:
                @pl.when((chip == 1) & (k_left >= 0) & (k_left < early))
                def _():
                    finish(k_left)

            if early_left and i == chips - 3:
                @pl.when((chip == chips - 2) & (k_right >= 0) & (k_right < early_left))
                def _():
                    finish(k_right)

        each(0, chunks + lag, one)

    done = jnp.where(chip == chips - 2, early_left, 0)
    each(jnp.where(chip == 1, early, done), chunks, finish)

    @pl.when(sec == sections - 1)
    def _():
        out_ref[...] = jnp.zeros_like(out_ref)

    def sent(part, sem):
        pltpu.make_async_copy(part, part, sem).wait()

    with jax.named_scope('drain'):
        for c in range(chips):
            @pl.when(chip == c)
            def _():
                pieces = kvh * ((2 if c < last else 0) + 1) + (2 if direct and c == last - 2 else 0)
                sent(q_all.at[:, :pieces * HD], kv_sent.at[0])
                relays = kvh * min(c, reach - 1) if c < last else 0
                relays -= 1 if direct and c == last - 1 else 0
                if relays:
                    sent(q_all.at[:, :2 * relays * HD], kv_passed.at[0])

        for which in range(2):
            qo_partner(which).wait_send()
        w_copy.wait_send()

        @pl.when(chip // (chips // 2) == core)
        def _():
            sent(dq_buf.at[:units - chip_heads // group // 2], dq_sent.at[0])

        @pl.when(chip // (chips // 2) != core)
        def _():
            sent(dq_buf, dq_sent.at[0])

        for e in range(reach + 1):
            @pl.when(chip >= e)
            def _():
                kvg_copy(e).wait_send()

        for c in range(chips):
            @pl.when(chip == c)
            def _():
                if c < last:
                    sent(right_buf.at[c + 1:], right_sent.at[0])
                if c > 0:
                    sent(left_buf.at[:c], left_sent.at[0])

        @pl.when(sec > 0)
        def _():
            sent(final, final_sent.at[0])

        @pl.when(sec < sections - 1)
        def _():
            got(final, final_got.at[0])


def body(queries, keys, values, out_grad, documents, query_weight, key_weight, value_weight):
    sections = lax.axis_size("section")
    count = lax.axis_size("seq")
    tok = queries.shape[1]
    total = tok * count
    kv = keys.shape[2] // HD
    feats = query_weight.shape[1]
    heads = feats // HD
    width = query_weight.shape[2]
    chips = count // 2
    rows = 2 * tok
    reach = -(-(total // 2) // rows)
    group = 2
    cw = min(256, width)
    chunks = width // cw
    units = chips * heads // group
    kvh = kv // 2
    slots = (reach + 1) * rows
    dma = pltpu.SemaphoreType.DMA
    anywhere = pl.BlockSpec(memory_space=pl.ANY)
    vmem = pl.BlockSpec(memory_space=pltpu.VMEM)
    out = pl.pallas_call(
        functools.partial(kernel, (sections, count, tok, heads, kv, width, cw, group, reach)),
        out_shape=pltpu.VMEM((tok, width), BF16),
        in_specs=[anywhere] * 8,
        out_specs=vmem,
        scratch_shapes=[
            pltpu.VMEM((1, total), jnp.int32),
            pltpu.VMEM((rows, chips * feats), BF16),
            pltpu.VMEM((rows, chips * feats), BF16),
            pltpu.VMEM((2, tok, kv * HD), BF16),
            pltpu.VMEM((2, kvh, slots, HD), BF16),
            pltpu.VMEM((HD, slots), BF16),
            pltpu.VMEM((slots, rows), F32),
            pltpu.VMEM((slots, HD), F32),
            pltpu.VMEM((slots, HD), F32),
            pltpu.VMEM((units, rows, group * HD), BF16),
            pltpu.VMEM((chips, tok, 2 * feats), BF16),
            pltpu.VMEM((reach + 1, 2, tok, 2 * kv * HD), BF16),
            pltpu.VMEM((2 * feats, width), BF16),
            pltpu.VMEM((2 * kv * HD, width), BF16),
            pltpu.VMEM((chips, chunks, tok, cw), BF16),
            pltpu.VMEM((chips, chunks, tok, cw), BF16),
            pltpu.VMEM((tok, cw), F32),
            pltpu.VMEM((chunks, tok, cw), BF16),
            dma((1,)),
            dma((2,)),
            dma((2,)),
            dma((2,)),
            dma((1,)),
            dma((2, kvh, reach + 1)),
            dma((1,)),
            dma((2,)),
            dma((1,)),
            dma((1,)),
            dma((1,)),
            dma((chips,)),
            dma((reach + 1,)),
            dma((reach + 1,)),
            dma((1,)),
            dma((max(chips - 2, 1), chunks)),
            dma((1,)),
            dma((max(chips - 2, 1), chunks)),
            dma((chunks,)),
            dma((1,)),
            dma((1,)),
            dma((1,)),
        ],
        compiler_params=pltpu.CompilerParams(
            collective_id=0, has_side_effects=True, vmem_limit_bytes=60 * 1024 * 1024),
        name="attention_back",
    )(queries[0], keys[0], values[0], out_grad[0], documents,
      query_weight[0], key_weight[0], value_weight[0])
    return out[None]


def solution(mesh):
    in_specs = (
        P("section", "seq", None),
        P("section", "seq", None),
        P("section", "seq", None),
        P("section", "seq", None),
        P("section", None),
        P("section", "seq", None),
        P("section", None, None),
        P("section", None, None),
    )
    out_specs = P("section", "seq", None)
    return jax.shard_map(body, mesh=mesh, in_specs=in_specs, out_specs=out_specs, check_vma=False)
```
